32 devices in a mesh: ctx: 16 (over z, y, core), fsdp: 2 (over x).
Axes of the slice: x: 2, y: 2, z: 4, core: 2. Of those that a mesh axis runs over, the one named last changes fastest.
Arguments:
- residual_in: bfloat16 [4096, 1024], P(('ctx', 'fsdp')), may hold values from -6 to 6
- first_gain: bfloat16 [1024], P(('ctx', 'fsdp')), may hold values from 0.5 to 1.5
- first_shift: bfloat16 [1024], P(('ctx', 'fsdp')), may hold values from -3 to 3
- attend_weight: bfloat16 [1024, 3072], P(('ctx', 'fsdp')), may hold values from -0.1875 to 0.1875
- attend_bias: bfloat16 [2048], P(('ctx', 'fsdp')), may hold values from -0.59765625 to 0.59765625
- merge_weight: bfloat16 [1024, 1024], P(('ctx', 'fsdp')), may hold values from -3 to 3
- merge_bias: bfloat16 [1024], P(('ctx', 'fsdp')), may hold values from -3 to 3
- second_gain: bfloat16 [1024], P(('ctx', 'fsdp')), may hold values from 0.5 to 1.5
- second_shift: bfloat16 [1024], P(('ctx', 'fsdp')), may hold values from -3 to 3
- expand_weight: bfloat16 [1024, 4096], P(('ctx', 'fsdp')), may hold values from -0.1875 to 0.1875
- expand_bias: bfloat16 [4096], P(('ctx', 'fsdp')), may hold values from -3 to 3
- shrink_weight: bfloat16 [4096, 1024], P(('ctx', 'fsdp')), may hold values from -0.09375 to 0.09375
- shrink_bias: bfloat16 [1024], P(('ctx', 'fsdp')), may hold values from -3 to 3
- cotangent: bfloat16 [4096, 1024], P(('ctx', 'fsdp')), may hold values from -6 to 6
Outputs:
- residual_out: bfloat16 [4096, 1024], P(('ctx', 'fsdp'))
- input_grad: float32 [4096, 1024], P(('ctx', 'fsdp'))
- grad_first_gain: float32 [1024], P(('ctx', 'fsdp'))
- grad_first_shift: float32 [1024], P(('ctx', 'fsdp'))
- grad_attend_weight: float32 [1024, 3072], P(('ctx', 'fsdp'))
- grad_attend_bias: float32 [2048], P(('ctx', 'fsdp'))
- grad_merge_weight: float32 [1024, 1024], P(('ctx', 'fsdp'))
- grad_merge_bias: float32 [1024], P(('ctx', 'fsdp'))
- grad_second_gain: float32 [1024], P(('ctx', 'fsdp'))
- grad_second_shift: float32 [1024], P(('ctx', 'fsdp'))
- grad_expand_weight: float32 [1024, 4096], P(('ctx', 'fsdp'))
- grad_expand_bias: float32 [4096], P(('ctx', 'fsdp'))
- grad_shrink_weight: float32 [4096, 1024], P(('ctx', 'fsdp'))
- grad_shrink_bias: float32 [1024], P(('ctx', 'fsdp'))
The draws below stay inside these ranges and needn't reach their ends.
All inputs are finite; a program needn't handle non-finite values.
Results may differ from the reference program's by a relative error of at most 0.014.
Values may be sent and summed in bfloat16 or wider, within the bound.
A program may use at most 384 MiB of HBM per device.

```python
import math
import jax
import jax.numpy as jnp
from jax import lax

D = 1024
H = 16
DH = 64
FF = 4096
TOKENS = 4096


def with_spikes(array, key, source, target, shards_of, factor):
    def block_of(position):
        return (jnp.arange(array.shape[position]) // (array.shape[position] // shards_of)).reshape((-1,) + (1,) * (array.ndim - 1 - position))

    near = jax.random.permutation(key, shards_of)[block_of(target)]
    second = (block_of(target) + shards_of // 2) % shards_of
    return jnp.where((block_of(source) == near) | (block_of(source) == second), factor * array, array)


def steps_of(rng, shape, split, low, largest):
    factor_of = 1.0
    for axis_at, shards_of in split:
        steps = jax.random.uniform(jax.random.fold_in(jax.random.fold_in(rng, 6), axis_at), (shards_of,), jnp.float32, low / len(split), largest / len(split))
        factor_of = factor_of * jnp.repeat(jnp.exp(steps), shape[axis_at] // shards_of).reshape((-1,) + (1,) * (len(shape) - 1 - axis_at))
    return factor_of


def scatter_about(own_key, shape, spread, most, shards=(), held_as=jnp.bfloat16):
    values = spread * jax.random.normal(own_key, shape, jnp.float32)
    if shards:
        values = values * steps_of(own_key, shape, shards, -0.22, 0.18)
    return jnp.clip(values, -most, most).astype(held_as)


def noise_with(rng, extent, deviation, bound, pieces, heavy, kind=jnp.bfloat16):
    array = deviation * jax.random.normal(rng, extent, jnp.float32)
    if pieces:
        array = array * steps_of(rng, extent, pieces, -0.22, 0.18)
    return jnp.clip(with_spikes(array, jax.random.fold_in(rng, 3), *heavy), -bound, bound).astype(kind)


def setup_inputs(seed: int = 0) -> dict:
    seeds = jax.random.split(jax.random.key(seed), 15)
    return {
        "residual_in": scatter_about(seeds[0], (TOKENS, D), 1.0, 6.0, ((0, 32),)),
        "first_gain": jnp.clip(1.0 + 0.1 * jax.random.normal(seeds[1], (D,), jnp.float32), 0.5, 1.5).astype(jnp.bfloat16),
        "first_shift": scatter_about(seeds[2], (D,), 0.5, 3.0, ((0, 32),)),
        "attend_weight": scatter_about(seeds[3], (D, 3 * D), D ** -0.5, 0.1875, ((0, 32),)),
        "attend_bias": scatter_about(seeds[4], (2 * D,), 0.1, 0.59765625, ((0, 32),)),
        "merge_weight": scatter_about(seeds[5], (D, D), 0.5, 3.0, ((0, 32),)),
        "merge_bias": scatter_about(seeds[6], (D,), 0.5, 3.0, ((0, 32),)),
        "second_gain": jnp.clip(1.0 + 0.1 * jax.random.normal(seeds[7], (D,), jnp.float32), 0.5, 1.5).astype(jnp.bfloat16),
        "second_shift": scatter_about(seeds[8], (D,), 0.5, 3.0, ((0, 32),)),
        "expand_weight": scatter_about(seeds[9], (D, FF), D ** -0.5, 0.1875, ((0, 32),)),
        "expand_bias": scatter_about(seeds[10], (FF,), 0.5, 3.0, ((0, 32),)),
        "shrink_weight": scatter_about(seeds[11], (FF, D), FF ** -0.5, 0.09375, ((0, 32),)),
        "shrink_bias": scatter_about(seeds[12], (D,), 0.5, 3.0, ((0, 32),)),
        "cotangent": noise_with(seeds[13], (TOKENS, D), 1.0, 6.0, ((0, 32),), (0, 1, 32, 2.75)),
    }


EPSILON = 1e-05
GELU_SCALE = 0.7978845608028654
GELU_CUBIC = 0.044715

def normalize(inputs, gain_row, shift_row):
    centred = inputs - lax.optimization_barrier(jnp.mean(inputs, axis=1, keepdims=True))
    inverse = lax.rsqrt(lax.optimization_barrier(jnp.mean(centred * centred, axis=1, keepdims=True)) + EPSILON)
    scaled = centred * inverse
    return (scaled, inverse, scaled * gain_row + shift_row)

def normalize_back(grad_norm, scaled, inverse, gain_row):
    grad_scaled = grad_norm * gain_row
    mean_one = lax.optimization_barrier(jnp.mean(grad_scaled, axis=1, keepdims=True))
    mean_two = lax.optimization_barrier(jnp.mean(grad_scaled * scaled, axis=1, keepdims=True))
    grad_inputs = inverse * (grad_scaled - mean_one - scaled * mean_two)
    return (grad_inputs, lax.optimization_barrier(jnp.sum(grad_norm * scaled, axis=0)), lax.optimization_barrier(jnp.sum(grad_norm, axis=0)))

def gelu_pair(pre_act):
    tangent = jnp.tanh(GELU_SCALE * (pre_act + GELU_CUBIC * pre_act * pre_act * pre_act))
    activated = 0.5 * pre_act * (1.0 + tangent)
    derivative = 0.5 * (1.0 + tangent) + 0.5 * pre_act * (1.0 - tangent * tangent) * GELU_SCALE * (1.0 + 3.0 * GELU_CUBIC * pre_act * pre_act)
    return (activated, derivative)

def block_layout():
    block_size = math.gcd(256, TOKENS)
    return (block_size, TOKENS // block_size)

def attention_forward(queries, key_rows, value_rows):
    block_size, block_count = block_layout()
    scaling = 1.0 / math.sqrt(DH)
    key_heads = key_rows.reshape(TOKENS, H, DH).astype(jnp.float32)
    value_heads = value_rows.reshape(TOKENS, H, DH).astype(jnp.float32)
    key_pos = jnp.arange(TOKENS, dtype=jnp.int32)

    def one_block(element):
        query_block, block_start = element
        scores = jnp.einsum('qhd,khd->hqk', query_block.astype(jnp.float32), key_heads) * scaling
        query_pos = block_start + jnp.arange(block_size, dtype=jnp.int32)
        allowed = key_pos[None, :] <= query_pos[:, None]
        scores = jnp.where(allowed[None], scores, -jnp.inf)
        row_max = lax.optimization_barrier(jnp.max(scores, axis=2))
        weights = jnp.exp(scores - row_max[:, :, None])
        totals = lax.optimization_barrier(jnp.sum(weights, axis=2))
        rounded = lax.optimization_barrier(weights.astype(jnp.bfloat16)).astype(jnp.float32)
        summed = jnp.einsum('hqk,khd->hqd', rounded, value_heads)
        attended = (summed / totals[:, :, None]).transpose(1, 0, 2).reshape(block_size, D).astype(jnp.bfloat16)
        return (attended, (row_max + jnp.log(totals)).T)
    starts = jnp.arange(block_count, dtype=jnp.int32) * block_size
    attended, log_total = lax.map(one_block, (queries.reshape(block_count, block_size, H, DH), starts))
    return (attended.reshape(TOKENS, D), log_total.reshape(TOKENS, H))

def attention_backward(queries, key_rows, value_rows, grad_attended, log_total, row_delta):
    block_size, block_count = block_layout()
    scaling = 1.0 / math.sqrt(DH)
    key_heads = key_rows.reshape(TOKENS, H, DH).astype(jnp.float32)
    value_heads = value_rows.reshape(TOKENS, H, DH).astype(jnp.float32)
    key_pos = jnp.arange(TOKENS, dtype=jnp.int32)

    def one_block(running, element):
        query_block, grad_block, total_block, delta_block, block_start = element
        query_float = query_block.astype(jnp.float32)
        grad_float = grad_block.astype(jnp.float32)
        scores = jnp.einsum('qhd,khd->hqk', query_float, key_heads) * scaling
        query_pos = block_start + jnp.arange(block_size, dtype=jnp.int32)
        allowed = key_pos[None, :] <= query_pos[:, None]
        scores = jnp.where(allowed[None], scores, -jnp.inf)
        probs_full = jnp.exp(scores - total_block.T[:, :, None])
        rounded = lax.optimization_barrier(probs_full.astype(jnp.bfloat16)).astype(jnp.float32)
        grad_vals = running[1] + jnp.einsum('hqk,qhd->khd', rounded, grad_float)
        grad_probs = jnp.einsum('qhd,khd->hqk', grad_float, value_heads)
        grad_scores = probs_full * (grad_probs - delta_block.T[:, :, None]) * scaling
        rounded_scores = lax.optimization_barrier(grad_scores.astype(jnp.bfloat16)).astype(jnp.float32)
        grad_query = jnp.einsum('hqk,khd->qhd', rounded_scores, key_heads).reshape(block_size, D)
        grad_key = running[0] + jnp.einsum('hqk,qhd->khd', rounded_scores, query_float)
        return ((grad_key, grad_vals), grad_query)
    starts = jnp.arange(block_count, dtype=jnp.int32) * block_size
    zero_heads = jnp.zeros((TOKENS, H, DH), jnp.float32)
    elements = (queries.reshape(block_count, block_size, H, DH), grad_attended.reshape(block_count, block_size, H, DH), log_total.reshape(block_count, block_size, H), row_delta.reshape(block_count, block_size, H), starts)
    carried, grad_queries = lax.scan(one_block, (zero_heads, zero_heads), elements)
    return (grad_queries.reshape(TOKENS, D), carried[0].reshape(TOKENS, D), carried[1].reshape(TOKENS, D))

def reference(residual_in, first_gain, first_shift, attend_weight, attend_bias, merge_weight, merge_bias, second_gain, second_shift, expand_weight, expand_bias, shrink_weight, shrink_bias, cotangent):
    block_in = residual_in.astype(jnp.float32)
    scaled_one, inverse_one, normed_one = normalize(block_in, first_gain.astype(jnp.float32), first_shift.astype(jnp.float32))
    input_one = normed_one.astype(jnp.bfloat16)
    projected = jnp.dot(input_one, attend_weight, preferred_element_type=jnp.float32)
    bias_float = attend_bias.astype(jnp.float32)
    queries = (projected[:, :D] + bias_float[:D]).astype(jnp.bfloat16)
    key_rows = projected[:, D:2 * D].astype(jnp.bfloat16)
    value_rows = (projected[:, 2 * D:] + bias_float[D:]).astype(jnp.bfloat16)
    attended, log_total = attention_forward(queries, key_rows, value_rows)
    merged = jnp.dot(attended, merge_weight, preferred_element_type=jnp.float32) + merge_bias.astype(jnp.float32)
    hidden = block_in + merged
    scaled_two, inverse_two, normed_two = normalize(hidden, second_gain.astype(jnp.float32), second_shift.astype(jnp.float32))
    input_two = normed_two.astype(jnp.bfloat16)
    pre_act = jnp.dot(input_two, expand_weight, preferred_element_type=jnp.float32) + expand_bias.astype(jnp.float32)
    activated, derivative = gelu_pair(pre_act)
    act_input = activated.astype(jnp.bfloat16)
    residual_out = (hidden + jnp.dot(act_input, shrink_weight, preferred_element_type=jnp.float32) + shrink_bias.astype(jnp.float32)).astype(jnp.bfloat16)
    grad_top = cotangent.astype(jnp.float32)
    grad_shrink_bias = lax.optimization_barrier(jnp.sum(grad_top, axis=0))
    grad_shrink_weight = jnp.dot(act_input.T, cotangent, preferred_element_type=jnp.float32)
    grad_pre = jnp.dot(cotangent, shrink_weight.T, preferred_element_type=jnp.float32) * derivative
    grad_expand_bias = lax.optimization_barrier(jnp.sum(grad_pre, axis=0))
    grad_pre_input = grad_pre.astype(jnp.bfloat16)
    grad_expand_weight = jnp.dot(input_two.T, grad_pre_input, preferred_element_type=jnp.float32)
    grad_two = jnp.dot(grad_pre_input, expand_weight.T, preferred_element_type=jnp.float32)
    grad_norm_two, grad_second_gain, grad_second_shift = normalize_back(grad_two, scaled_two, inverse_two, second_gain.astype(jnp.float32))
    grad_hidden = grad_top + grad_norm_two
    grad_hidden_input = grad_hidden.astype(jnp.bfloat16)
    grad_merge_bias = lax.optimization_barrier(jnp.sum(grad_hidden, axis=0))
    grad_merge_weight = jnp.dot(attended.T, grad_hidden_input, preferred_element_type=jnp.float32)
    grad_attended = jnp.dot(grad_hidden_input, merge_weight.T, preferred_element_type=jnp.float32).astype(jnp.bfloat16)
    row_delta = lax.optimization_barrier(jnp.sum((grad_attended.astype(jnp.float32) * attended.astype(jnp.float32)).reshape(TOKENS, H, DH), axis=2))
    grad_queries, grad_keys, grad_values = attention_backward(queries, key_rows, value_rows, grad_attended, log_total, row_delta)
    grad_attend_bias = jnp.concatenate([lax.optimization_barrier(jnp.sum(grad_queries, axis=0)), lax.optimization_barrier(jnp.sum(grad_values, axis=0))])
    grad_projected = jnp.concatenate([grad_queries, grad_keys, grad_values], axis=1).astype(jnp.bfloat16)
    grad_attend_weight = jnp.dot(input_one.T, grad_projected, preferred_element_type=jnp.float32)
    grad_one = jnp.dot(grad_projected, attend_weight.T, preferred_element_type=jnp.float32)
    grad_norm_one, grad_first_gain, grad_first_shift = normalize_back(grad_one, scaled_one, inverse_one, first_gain.astype(jnp.float32))
    input_grad = grad_hidden + grad_norm_one
    return (residual_out, input_grad, grad_first_gain, grad_first_shift, grad_attend_weight, grad_attend_bias, grad_merge_weight, grad_merge_bias, grad_second_gain, grad_second_shift, grad_expand_weight, grad_expand_bias, grad_shrink_weight, grad_shrink_bias)
```

```python
import math

import jax
import jax.numpy as jnp
from jax import lax
from jax.experimental import pallas as pl
from jax.experimental.pallas import tpu as pltpu
from jax.sharding import PartitionSpec as P

H = 16
G = 8
EPSILON = 1e-05
GELU_SCALE = 0.7978845608028654
GELU_CUBIC = 0.044715
LOG2E = 1.4426950408889634
MESH = pl.DeviceIdType.MESH
BF16 = jnp.bfloat16
F32 = jnp.float32


def position(fsdp):
    return lax.axis_index("ctx") * fsdp + lax.axis_index("fsdp")


class Wire:
    def __init__(self, n, fsdp, send, recv, local):
        self.n, self.fsdp = n, fsdp
        self.send, self.recv, self.local = send, recv, local
        self.me = position(fsdp)
        self.t, self.m = self.me // G, lax.rem(self.me, G)

    def where(self, device):
        return (device // self.fsdp, lax.rem(device, self.fsdp))

    def greet(self):
        barrier = pltpu.get_barrier_semaphore()

        def hello(step, carry):
            other = lax.rem(self.me + step, self.n)
            pl.semaphore_signal(barrier, inc=1, device_id=self.where(other), device_id_type=MESH)
            return carry

        lax.fori_loop(1, self.n, hello, 0)
        pl.semaphore_wait(barrier, self.n - 1)

    def put(self, lane, source, target, device):
        pltpu.make_async_remote_copy(
            src_ref=source,
            dst_ref=target,
            send_sem=self.send.at[lane],
            recv_sem=self.recv.at[lane],
            device_id=self.where(device),
            device_id_type=MESH,
        ).start()

    def keep(self, lane, source, target):
        pltpu.make_async_copy(source, target, self.local.at[lane]).start()

    def kept(self, lane, like):
        pltpu.make_async_copy(like, like, self.local.at[lane]).wait()

    def sent(self, lane, like):
        pltpu.make_async_copy(like, like, self.send.at[lane]).wait()

    def came(self, lane, like):
        pltpu.make_async_copy(like, like, self.recv.at[lane]).wait()

    def settle(self, lane, like):
        self.came(lane, like)
        self.sent(lane, like)

    def group(self, step):
        m = lax.rem(self.m + step, G)
        return m, self.t * G + m

    def column(self, step, groups):
        t = lax.rem(self.t + step, groups)
        return t, t * G + self.m


def exchange(body, name, number, n, fsdp, lanes, inputs, outs):
    def kernel(*refs):
        ins = refs[: len(inputs)]
        results = refs[len(inputs) : len(inputs) + len(outs)]
        wire = Wire(n, fsdp, *refs[len(inputs) + len(outs) :])
        wire.greet()
        body(wire, *ins, *results)

    kernel.__name__ = name
    return pl.pallas_call(
        kernel,
        out_shape=[jax.ShapeDtypeStruct(shape, kind) for shape, kind in outs],
        in_specs=[pl.BlockSpec(memory_space=pltpu.VMEM)] * len(inputs),
        out_specs=[pl.BlockSpec(memory_space=pl.ANY)] * len(outs),
        scratch_shapes=[pltpu.SemaphoreType.DMA((lanes,))] * 3,
        compiler_params=pltpu.CompilerParams(collective_id=number, has_side_effects=True),
        name=name,
    )(*inputs)


def loop(low, high, step):
    def turn(index, carry):
        step(index)
        return carry

    lax.fori_loop(low, high, turn, 0)


def normalize(inputs):
    centred = inputs - jnp.mean(inputs, axis=1, keepdims=True)
    inverse = lax.rsqrt(jnp.mean(centred * centred, axis=1, keepdims=True) + EPSILON)
    return centred * inverse, inverse


def normalize_back(grad_norm, scaled, inverse, gain_row):
    grad_scaled = grad_norm * gain_row
    mean_one = jnp.mean(grad_scaled, axis=1, keepdims=True)
    mean_two = jnp.mean(grad_scaled * scaled, axis=1, keepdims=True)
    return inverse * (grad_scaled - mean_one - scaled * mean_two)


def gelu_pair(pre_act):
    tangent = jnp.tanh(GELU_SCALE * (pre_act + GELU_CUBIC * pre_act * pre_act * pre_act))
    activated = 0.5 * pre_act * (1.0 + tangent)
    derivative = 0.5 * (1.0 + tangent) + 0.5 * pre_act * (1.0 - tangent * tangent) * GELU_SCALE * (
        1.0 + 3.0 * GELU_CUBIC * pre_act * pre_act
    )
    return (activated, derivative)


def dot(left, right, left_dim, right_dim):
    return lax.dot_general(
        left, right, (((left_dim,), (right_dim,)), ((), ())), preferred_element_type=F32
    )


def tiles_of(queries, keys, parts):
    wide = min(256, queries)
    deep = min(512, wide * parts)
    return wide, deep, wide * parts // deep


def query_places(tile, wide, parts, part):
    column = lax.broadcasted_iota(jnp.int32, (1, wide), 1)
    block = tile * (wide // 128) + column // 128
    return (block * parts + part) * 128 + lax.rem(column, 128)


def attend(groups, fsdp, parts, query_t, pair_t):
    width, queries = query_t.shape
    keys = pair_t.shape[2]
    wide, deep, band = tiles_of(queries, keys, parts)
    factor = LOG2E / math.sqrt(width)

    def kernel(query_ref, pair_ref, out_ref, total_ref, key_ref):
        tile = pl.program_id(0)
        part = lax.rem(position(fsdp) // G, parts)

        @pl.when(tile == 0)
        def _():
            def turn(j):
                at = pl.ds(pl.multiple_of(j * deep, deep), deep)
                key_ref[at, :] = pair_ref[0, :, at].T

            loop(0, keys // deep, turn)

        query = query_ref[...]
        places = query_places(tile, wide, parts, part)

        def step(j, carry, masked):
            best, total, summed = carry
            at = pl.ds(pl.multiple_of(j * deep, deep), deep)
            scores = dot(key_ref[at, :], query, 1, 0)
            if masked:
                key_places = j * deep + lax.broadcasted_iota(jnp.int32, (deep, wide), 0)
                scores = jnp.where(key_places <= places, scores, -1e30)
            higher = jnp.maximum(best, jnp.max(scores, axis=0, keepdims=True))
            weights = jnp.exp2((scores - higher) * factor)
            shrunk = jnp.exp2((best - higher) * factor)
            total = total * shrunk + jnp.sum(weights, axis=0, keepdims=True)
            summed = summed * shrunk + dot(pair_ref[1, :, at], weights.astype(BF16), 1, 0)
            return higher, total, summed

        carry = (
            jnp.full((1, wide), -1e30, F32),
            jnp.zeros((1, wide), F32),
            jnp.zeros((width, wide), F32),
        )
        carry = lax.fori_loop(0, tile * band, lambda j, c: step(j, c, False), carry)
        for extra in range(band):
            carry = step(tile * band + extra, carry, True)
        best, total, summed = carry
        out_ref[...] = (summed / total).astype(BF16)
        total_ref[...] = best * factor + jnp.log2(total)

    across = pl.BlockSpec((width, wide), lambda i: (0, i))
    return pl.pallas_call(
        kernel,
        grid=(queries // wide,),
        out_shape=[
            jax.ShapeDtypeStruct((width, queries), BF16),
            jax.ShapeDtypeStruct((1, queries), F32),
        ],
        in_specs=[across, pl.BlockSpec((2, width, keys), lambda i: (0, 0, 0))],
        out_specs=[across, pl.BlockSpec((1, wide), lambda i: (0, i))],
        scratch_shapes=[pltpu.VMEM((keys, width), BF16)],
        name="attend",
    )(query_t, pair_t)


def attend_back(groups, fsdp, parts, query_t, pair_t, grad_t, out_t, total):
    width, queries = query_t.shape
    keys = pair_t.shape[2]
    wide, deep, band = tiles_of(queries, keys, parts)
    scale = 1.0 / math.sqrt(width)
    factor = LOG2E * scale

    def kernel(
        query_ref, pair_ref, grad_ref, out_ref, total_ref, dq_ref, dpair_ref, key_ref, value_ref, dkey_ref, dvalue_ref
    ):
        tile = pl.program_id(0)
        part = lax.rem(position(fsdp) // G, parts)

        @pl.when(tile == 0)
        def _():
            def turn(j):
                at = pl.ds(pl.multiple_of(j * deep, deep), deep)
                key_ref[at, :] = pair_ref[0, :, at].T
                value_ref[at, :] = pair_ref[1, :, at].T
                dkey_ref[at, :] = jnp.zeros((deep, width), F32)
                dvalue_ref[at, :] = jnp.zeros((deep, width), F32)

            loop(0, keys // deep, turn)

        query, grad = query_ref[...], grad_ref[...]
        query_rows, grad_rows = query.T, grad.T
        lse = total_ref[...]
        delta = jnp.sum(grad.astype(F32) * out_ref[...].astype(F32), axis=0, keepdims=True)
        places = query_places(tile, wide, parts, part)

        def step(j, summed, masked):
            at = pl.ds(pl.multiple_of(j * deep, deep), deep)
            scores = dot(key_ref[at, :], query, 1, 0) * factor
            if masked:
                key_places = j * deep + lax.broadcasted_iota(jnp.int32, (deep, wide), 0)
                scores = jnp.where(key_places <= places, scores, -1e30)
            probs = jnp.exp2(scores - lse)
            dvalue_ref[at, :] += dot(probs.astype(BF16), grad_rows, 1, 0)
            grad_probs = dot(value_ref[at, :], grad, 1, 0)
            grad_scores = (probs * (grad_probs - delta) * scale).astype(BF16)
            dkey_ref[at, :] += dot(grad_scores, query_rows, 1, 0)
            return summed + dot(pair_ref[0, :, at], grad_scores, 1, 0)

        summed = jnp.zeros((width, wide), F32)
        summed = lax.fori_loop(0, tile * band, lambda j, c: step(j, c, False), summed)
        for extra in range(band):
            summed = step(tile * band + extra, summed, True)
        dq_ref[...] = summed.astype(BF16)

        @pl.when(tile == pl.num_programs(0) - 1)
        def _():
            def turn(j):
                at = pl.ds(pl.multiple_of(j * deep, deep), deep)
                dpair_ref[0, :, at] = dkey_ref[at, :].T.astype(BF16)
                dpair_ref[1, :, at] = dvalue_ref[at, :].T.astype(BF16)

            loop(0, keys // deep, turn)

    across = pl.BlockSpec((width, wide), lambda i: (0, i))
    line = pl.BlockSpec((1, wide), lambda i: (0, i))
    whole = pl.BlockSpec((2, width, keys), lambda i: (0, 0, 0))
    return pl.pallas_call(
        kernel,
        grid=(queries // wide,),
        out_shape=[
            jax.ShapeDtypeStruct((width, queries), BF16),
            jax.ShapeDtypeStruct((2, width, keys), BF16),
        ],
        in_specs=[across, whole, across, across, line],
        out_specs=[across, whole],
        scratch_shapes=[
            pltpu.VMEM((keys, width), BF16),
            pltpu.VMEM((keys, width), BF16),
            pltpu.VMEM((keys, width), F32),
            pltpu.VMEM((keys, width), F32),
        ],
        name="attend_back",
    )(query_t, pair_t, grad_t, out_t, total)


def layer(n, fsdp):
    groups = n // G
    parts = groups // 2

    def on_device(
        residual_in,
        first_gain,
        first_shift,
        attend_weight,
        attend_bias,
        merge_weight,
        merge_bias,
        second_gain,
        second_shift,
        expand_weight,
        expand_bias,
        shrink_weight,
        shrink_bias,
        cotangent,
    ):
        rows, width = residual_in.shape
        depth = width // n
        hidden_rows = shrink_weight.shape[0]
        hidden_units = expand_weight.shape[1]
        slice_width = width // G
        slice_units = hidden_units // G
        head = width // H
        group_rows = rows * G
        tokens = rows * n
        queries = tokens // parts
        per_group = G // parts
        me = position(fsdp)
        member = lax.rem(me, G)

        small = (first_gain, first_shift, attend_bias, merge_bias, second_gain, second_shift, expand_bias, shrink_bias)
        sizes = [s.shape[0] for s in small]
        packed_rows = -(-sum(sizes) // 2048) * 16
        packed = jnp.pad(jnp.concatenate(small), (0, packed_rows * 128 - sum(sizes))).reshape(packed_rows, 128)

        def gather_first(wire, x, attend, merge, vec, x_all, attend_all, merge_all, vec_all):
            me, t, m = wire.me, wire.t, wire.m

            def to_group(step):
                _, device = wire.group(step)
                wire.put(0, x, x_all.at[m], device)

            def to_all(step):
                device = lax.rem(me + step, n)
                other = lax.rem(device, G)
                for p in range(3):
                    columns = pl.ds(pl.multiple_of(p * width + other * slice_width, 128), slice_width)
                    wire.put(1, attend.at[:, columns], attend_all.at[me, :, pl.ds(p * slice_width, slice_width)], device)
                wire.put(3, vec, vec_all.at[me], device)

            def to_column(step):
                _, device = wire.column(step, groups)
                wire.put(2, merge, merge_all.at[t], device)

            loop(1, G, to_group)
            loop(1, n, to_all)
            loop(1, groups, to_column)
            wire.keep(0, x, x_all.at[m])
            for p in range(3):
                columns = pl.ds(pl.multiple_of(p * width + m * slice_width, 128), slice_width)
                wire.keep(1, attend.at[:, columns], attend_all.at[me, :, pl.ds(p * slice_width, slice_width)])
            wire.keep(2, merge, merge_all.at[t])
            wire.keep(3, vec, vec_all.at[me])
            wire.kept(0, x_all.at[0])
            wire.kept(1, attend_all.at[0])
            wire.kept(2, merge_all.at[0])
            wire.kept(3, vec_all.at[0])
            wire.settle(0, x_all.at[pl.ds(0, G - 1)])
            wire.settle(1, attend_all.at[pl.ds(0, n - 1)])
            wire.settle(2, merge_all.at[pl.ds(0, groups - 1)])
            wire.settle(3, vec_all.at[pl.ds(0, n - 1)])

        x_all, attend_all, merge_all, vec_all = exchange(
            gather_first,
            "gather_first",
            0,
            n,
            fsdp,
            4,
            (residual_in, attend_weight, merge_weight, packed),
            (
                ((G, rows, width), BF16),
                ((n, depth, 3 * slice_width), BF16),
                ((groups, depth, width), BF16),
                ((n, packed_rows, 128), BF16),
            ),
        )
        flat = vec_all.reshape(n, packed_rows * 128)
        spots = [sum(sizes[:k]) for k in range(len(sizes))]
        gain_one, shift_one, attend_shift, merge_shift, gain_two, shift_two, expand_shift, shrink_shift = (
            flat[:, spot : spot + size].reshape(-1).astype(F32) for spot, size in zip(spots, sizes)
        )
        attend_slice = attend_all.reshape(width, 3 * slice_width)

        scaled_group, _ = normalize(x_all.reshape(group_rows, width).astype(F32))
        input_one = (scaled_group * gain_one + shift_one).astype(BF16)
        bias_mine = jnp.concatenate(
            [
                lax.dynamic_slice_in_dim(attend_shift, member * slice_width, slice_width),
                jnp.zeros((slice_width,), F32),
                lax.dynamic_slice_in_dim(attend_shift, width + member * slice_width, slice_width),
            ]
        )
        projected = (dot(attend_slice, input_one, 0, 1) + bias_mine[:, None]).astype(BF16)
        projected = projected.reshape(3, 2, head, group_rows)

        def spread_heads(wire, qkv, merge, pair, query, merge_full):
            t, m = wire.t, wire.m

            def to_column(step, own=False):
                other, device = wire.column(step, groups)
                which, part = other // parts, lax.rem(other, parts)
                move = (lambda lane, s, d: wire.keep(lane, s, d)) if own else (lambda lane, s, d: wire.put(lane, s, d, device))
                mine = pl.ds(pl.multiple_of(t * group_rows, 128), group_rows)
                move(0, qkv.at[1, which], pair.at[0, :, mine])
                move(0, qkv.at[2, which], pair.at[1, :, mine])
                for i in range(per_group):
                    source = pl.ds(pl.multiple_of((part + i * parts) * rows, 128), rows)
                    target = pl.ds(pl.multiple_of((t * per_group + i) * rows, 128), rows)
                    move(1, qkv.at[0, which, :, source], query.at[:, target])

            def to_group(step):
                _, device = wire.group(step)
                wire.put(2, merge, merge_full.at[:, m], device)

            loop(1, groups, to_column)
            loop(1, G, to_group)
            to_column(0, own=True)
            wire.keep(2, merge, merge_full.at[:, m])
            wire.kept(0, pair.at[:, :, pl.ds(0, group_rows)])
            wire.kept(1, query.at[:, pl.ds(0, per_group * rows)])
            wire.kept(2, merge_full.at[:, 0])
            wire.settle(0, pair.at[:, :, pl.ds(0, tokens - group_rows)])
            wire.settle(1, query.at[:, pl.ds(0, queries - per_group * rows)])
            wire.settle(2, merge_full.at[:, pl.ds(0, G - 1)])

        pair_t, query_t, merge_full = exchange(
            spread_heads,
            "spread_heads",
            1,
            n,
            fsdp,
            3,
            (projected, merge_all),
            (((2, head, tokens), BF16), ((head, queries), BF16), ((groups, G, depth, width), BF16)),
        )
        merge_full = merge_full.reshape(width, width)
        out_t, log_total = attend(groups, fsdp, parts, query_t, pair_t)

        def send_attended(wire, out, attended):
            me, part = wire.me, lax.rem(wire.t, parts)
            place = pl.ds(pl.multiple_of((2 * wire.m + wire.t // parts) * head, head), head)

            def to_owner(k):
                device = k * parts + part
                source = out.at[:, pl.ds(pl.multiple_of(k * rows, 128), rows)]

                @pl.when(device != me)
                def _():
                    wire.put(0, source, attended.at[place, :], device)

                @pl.when(device == me)
                def _():
                    wire.keep(0, source, attended.at[place, :])

            loop(0, n // parts, to_owner)
            mine = lax.rem(me, parts) == part

            @pl.when(mine)
            def _():
                wire.kept(0, attended.at[pl.ds(0, head), :])
                wire.came(0, attended.at[pl.ds(0, width - head), :])
                wire.sent(0, out.at[:, pl.ds(0, queries - rows)])

            @pl.when(jnp.logical_not(mine))
            def _():
                wire.came(0, attended)
                wire.sent(0, out)

        (attended_t,) = exchange(send_attended, "send_attended", 2, n, fsdp, 1, (out_t,), (((width, rows), BF16),))

        block_in = residual_in.astype(F32)
        hidden = block_in + (dot(attended_t, merge_full, 0, 0) + merge_shift)
        scaled_two, inverse_two = normalize(hidden)
        input_two = (scaled_two * gain_two + shift_two).astype(BF16)

        def gather_second(wire, normed, cot, expand, shrink, normed_all, cot_all, expand_all, shrink_all):
            me, t, m = wire.me, wire.t, wire.m
            user = me // groups
            slot = lax.rem(me, groups)

            def to_group(step):
                _, device = wire.group(step)
                wire.put(0, normed, normed_all.at[m], device)

            def to_all(step):
                device = lax.rem(me + step, n)
                columns = pl.ds(pl.multiple_of(lax.rem(device, G) * slice_units, 128), slice_units)
                wire.put(2, expand.at[:, columns], expand_all.at[me], device)

            def to_users(step):
                other = lax.rem(t + step, groups)
                device = other * G + user

                @pl.when(device != me)
                def _():
                    wire.put(3, shrink, shrink_all.at[slot], device)

                @pl.when(device == me)
                def _():
                    wire.keep(3, shrink, shrink_all.at[slot])

            def cot_to_group(step):
                _, device = wire.group(step)
                wire.put(1, cot, cot_all.at[m], device)

            loop(1, G, to_group)
            loop(0, groups, to_users)
            loop(1, n, to_all)
            loop(1, G, cot_to_group)
            wire.keep(0, normed, normed_all.at[m])
            wire.keep(1, cot, cot_all.at[m])
            wire.keep(2, expand.at[:, pl.ds(pl.multiple_of(m * slice_units, 128), slice_units)], expand_all.at[me])
            wire.kept(0, normed_all.at[0])
            wire.kept(1, cot_all.at[0])
            wire.kept(2, expand_all.at[0])
            wire.settle(0, normed_all.at[pl.ds(0, G - 1)])
            wire.settle(1, cot_all.at[pl.ds(0, G - 1)])
            wire.settle(2, expand_all.at[pl.ds(0, n - 1)])

            @pl.when(user == m)
            def _():
                wire.kept(3, shrink_all.at[0])
                wire.settle(3, shrink_all.at[pl.ds(0, groups - 1)])

            @pl.when(user != m)
            def _():
                wire.settle(3, shrink_all)

        normed_all, cot_all, expand_all, shrink_all = exchange(
            gather_second,
            "gather_second",
            3,
            n,
            fsdp,
            4,
            (input_two, cotangent, expand_weight, shrink_weight),
            (
                ((G, rows, width), BF16),
                ((G, rows, width), BF16),
                ((n, depth, slice_units), BF16),
                ((groups, hidden_rows, width), BF16),
            ),
        )
        group_two = normed_all.reshape(group_rows, width)
        group_cot = cot_all.reshape(group_rows, width)
        expand_slice = expand_all.reshape(width, slice_units)
        shrink_slice = shrink_all.reshape(slice_units, width)
        shift_units = lax.dynamic_slice_in_dim(expand_shift, member * slice_units, slice_units)
        activated, derivative = gelu_pair(dot(group_two, expand_slice, 1, 0) + shift_units)
        act_input = activated.astype(BF16)
        shrunk_part = dot(act_input, shrink_slice, 1, 0).astype(BF16)
        grad_shrink_part = dot(act_input, group_cot, 0, 0).astype(BF16)
        grad_pre = dot(group_cot, shrink_slice, 1, 1) * derivative
        grad_expand_shift = jnp.sum(grad_pre, axis=0)
        grad_pre_input = grad_pre.astype(BF16)
        grad_expand_part = dot(group_two, grad_pre_input, 0, 0).astype(BF16)
        grad_two_part = dot(grad_pre_input, expand_slice, 1, 1).astype(BF16)

        def scatter_second(wire, two, shrunk, expand, shrink, two_all, shrunk_all, expand_all, shrink_all):
            me, t, m = wire.me, wire.t, wire.m
            columns = pl.ds(pl.multiple_of(m * slice_units, 128), slice_units)

            def to_group(step):
                other, device = wire.group(step)
                wire.put(0, two.at[other], two_all.at[m], device)

            def shrunk_to_group(step):
                other, device = wire.group(step)
                wire.put(1, shrunk.at[other], shrunk_all.at[m], device)

            def to_all(step):
                device = lax.rem(me + step, n)
                wire.put(2, expand.at[device], expand_all.at[t, :, columns], device)

            def to_owners(slot):
                device = m * groups + slot

                @pl.when(device != me)
                def _():
                    wire.put(3, shrink.at[slot], shrink_all.at[t], device)

                @pl.when(device == me)
                def _():
                    wire.keep(3, shrink.at[slot], shrink_all.at[t])

            loop(1, G, to_group)
            loop(0, groups, to_owners)
            loop(1, n, to_all)
            loop(1, G, shrunk_to_group)
            wire.keep(0, two.at[m], two_all.at[m])
            wire.keep(1, shrunk.at[m], shrunk_all.at[m])
            wire.keep(2, expand.at[me], expand_all.at[t, :, columns])
            wire.kept(0, two_all.at[0])
            wire.kept(1, shrunk_all.at[0])
            wire.kept(2, expand.at[0])
            wire.settle(0, two_all.at[pl.ds(0, G - 1)])
            wire.settle(1, shrunk_all.at[pl.ds(0, G - 1)])
            wire.settle(2, expand.at[pl.ds(0, n - 1)])

            @pl.when(me // groups == m)
            def _():
                wire.kept(3, shrink_all.at[0])
                wire.settle(3, shrink_all.at[pl.ds(0, groups - 1)])

            @pl.when(me // groups != m)
            def _():
                wire.settle(3, shrink_all)

        two_parts, shrunk_parts, expand_parts, shrink_parts = exchange(
            scatter_second,
            "scatter_second",
            4,
            n,
            fsdp,
            4,
            (
                grad_two_part.reshape(G, rows, width),
                shrunk_part.reshape(G, rows, width),
                grad_expand_part.reshape(n, depth, slice_units),
                grad_shrink_part.reshape(groups, hidden_rows, width),
            ),
            (
                ((G, rows, width), BF16),
                ((G, rows, width), BF16),
                ((groups, depth, hidden_units), BF16),
                ((groups, hidden_rows, width), BF16),
            ),
        )
        residual_out = (hidden + jnp.sum(shrunk_parts.astype(F32), axis=0) + shrink_shift).astype(BF16)
        grad_expand_weight = jnp.sum(expand_parts.astype(F32), axis=0)
        grad_shrink_weight = jnp.sum(shrink_parts.astype(F32), axis=0)

        grad_top = cotangent.astype(F32)
        grad_shrink_shift = jnp.sum(grad_top, axis=0)
        grad_two = jnp.sum(two_parts.astype(F32), axis=0)
        grad_gain_two = jnp.sum(grad_two * scaled_two, axis=0)
        grad_shift_two = jnp.sum(grad_two, axis=0)
        grad_hidden = grad_top + normalize_back(grad_two, scaled_two, inverse_two, gain_two)
        grad_merge_shift = jnp.sum(grad_hidden, axis=0)
        grad_hidden_input = grad_hidden.astype(BF16)
        grad_attended_t = dot(merge_full, grad_hidden_input, 1, 1).astype(BF16)

        def send_grad(wire, grad, grad_out):
            me = wire.me
            part, place = lax.rem(me, parts), pl.ds(pl.multiple_of(me // parts * rows, 128), rows)

            def to_head(h):
                device = (lax.rem(h, 2) * parts + part) * G + h // 2
                source = grad.at[pl.ds(pl.multiple_of(h * head, head), head), :]

                @pl.when(device != me)
                def _():
                    wire.put(0, source, grad_out.at[:, place], device)

                @pl.when(device == me)
                def _():
                    wire.keep(0, source, grad_out.at[:, place])

            loop(0, H, to_head)
            mine = lax.rem(wire.t, parts) == part

            @pl.when(mine)
            def _():
                wire.kept(0, grad.at[pl.ds(0, head), :])
                wire.came(0, grad_out.at[:, pl.ds(0, queries - rows)])
                wire.sent(0, grad.at[pl.ds(0, width - head), :])

            @pl.when(jnp.logical_not(mine))
            def _():
                wire.came(0, grad_out)
                wire.sent(0, grad)

        (grad_t,) = exchange(send_grad, "send_grad", 5, n, fsdp, 1, (grad_attended_t,), (((head, queries), BF16),))
        grad_query_t, grad_pair_t = attend_back(groups, fsdp, parts, query_t, pair_t, grad_t, out_t, log_total)

        def return_heads(wire, dq, dpair, grad, att, dq_all, dpair_all, grad_all, att_all):
            t, m = wire.t, wire.m
            which, part = t // parts, lax.rem(t, parts)

            def to_column(step, own=False):
                other, device = wire.column(step, groups)
                move = (lambda lane, s, d: wire.keep(lane, s, d)) if own else (lambda lane, s, d: wire.put(lane, s, d, device))
                theirs = pl.ds(pl.multiple_of(other * group_rows, 128), group_rows)
                move(0, dpair.at[:, :, theirs], dpair_all.at[part, which])
                for i in range(per_group):
                    source = pl.ds(pl.multiple_of((other * per_group + i) * rows, 128), rows)
                    target = pl.ds(pl.multiple_of((part + i * parts) * rows, 128), rows)
                    move(1, dq.at[:, source], dq_all.at[which, :, target])

            def to_group(step):
                other, device = wire.group(step)
                wire.put(2, grad, grad_all.at[m], device)
                wire.put(
                    3,
                    att.at[pl.ds(pl.multiple_of(other * slice_width, 128), slice_width), :],
                    att_all.at[:, pl.ds(pl.multiple_of(m * rows, 128), rows)],
                    device,
                )

            loop(1, groups, to_column)
            loop(1, G, to_group)
            to_column(0, own=True)
            wire.keep(2, grad, grad_all.at[m])
            wire.keep(
                3,
                att.at[pl.ds(pl.multiple_of(m * slice_width, 128), slice_width), :],
                att_all.at[:, pl.ds(pl.multiple_of(m * rows, 128), rows)],
            )
            wire.kept(0, dpair.at[:, :, pl.ds(0, group_rows)])
            wire.kept(1, dq.at[:, pl.ds(0, per_group * rows)])
            wire.kept(2, grad_all.at[0])
            wire.kept(3, att_all.at[:, pl.ds(0, rows)])
            wire.settle(0, dpair.at[:, :, pl.ds(0, tokens - group_rows)])
            wire.settle(1, dq.at[:, pl.ds(0, queries - per_group * rows)])
            wire.settle(2, grad_all.at[pl.ds(0, G - 1)])
            wire.settle(3, att_all.at[:, pl.ds(0, group_rows - rows)])

        dq_all, dpair_all, grad_all, att_all = exchange(
            return_heads,
            "return_heads",
            6,
            n,
            fsdp,
            4,
            (grad_query_t, grad_pair_t, grad_hidden_input, attended_t),
            (
                ((2, head, group_rows), BF16),
                ((parts, 2, 2, head, group_rows), BF16),
                ((G, rows, width), BF16),
                ((slice_width, group_rows), BF16),
            ),
        )
        grad_pair = jnp.sum(dpair_all.astype(F32), axis=0)
        grad_projected = jnp.concatenate(
            [
                dq_all.astype(F32).reshape(slice_width, group_rows),
                grad_pair[:, 0].reshape(slice_width, group_rows),
                grad_pair[:, 1].reshape(slice_width, group_rows),
            ],
            axis=0,
        )
        grad_shift_mine = jnp.sum(grad_projected, axis=1)
        grad_projected = grad_projected.astype(BF16)
        grad_attend_part = dot(input_one, grad_projected, 0, 1).astype(BF16)
        grad_one_part = dot(grad_projected, attend_slice, 0, 1)
        grad_gain_one = jnp.sum(grad_one_part * scaled_group, axis=0)
        grad_shift_one = jnp.sum(grad_one_part, axis=0)
        grad_merge_part = dot(att_all, grad_all.reshape(group_rows, width), 1, 0).astype(BF16)

        grad_attend_shift = jnp.zeros((2 * width,), F32)
        grad_attend_shift = lax.dynamic_update_slice_in_dim(
            grad_attend_shift, grad_shift_mine[:slice_width], member * slice_width, 0
        )
        grad_attend_shift = lax.dynamic_update_slice_in_dim(
            grad_attend_shift, grad_shift_mine[2 * slice_width :], width + member * slice_width, 0
        )
        grad_expand_all = lax.dynamic_update_slice_in_dim(
            jnp.zeros((hidden_units,), F32), grad_expand_shift, member * slice_units, 0
        )
        grads = (
            grad_gain_one,
            grad_shift_one,
            grad_attend_shift,
            grad_merge_shift,
            grad_gain_two,
            grad_shift_two,
            grad_expand_all,
            grad_shrink_shift,
        )
        total_size = sum(sizes)
        vec_rows = -(-total_size // 1024) * 8
        packed_grads = jnp.pad(
            jnp.concatenate([g.reshape(n, -1) for g in grads], axis=1), ((0, 0), (0, vec_rows * 128 - total_size))
        ).reshape(n, vec_rows, 128)

        def scatter_first(wire, one, attend, merge, vec, one_all, attend_all, merge_all, vec_all):
            me, t, m = wire.me, wire.t, wire.m

            def to_group(step):
                other, device = wire.group(step)
                wire.put(0, one.at[other], one_all.at[m], device)

            def attend_to(device, move):
                for p in range(3):
                    columns = pl.ds(pl.multiple_of(p * width + m * slice_width, 128), slice_width)
                    move(1, attend.at[device, :, pl.ds(p * slice_width, slice_width)], attend_all.at[t, :, columns])

            def to_all(step):
                device = lax.rem(me + step, n)
                attend_to(device, lambda lane, s, d: wire.put(lane, s, d, device))
                wire.put(3, vec.at[device], vec_all.at[me], device)

            def to_owners(slot):
                device = m * groups + slot

                @pl.when(device != me)
                def _():
                    wire.put(2, merge.at[slot], merge_all.at[t], device)

                @pl.when(device == me)
                def _():
                    wire.keep(2, merge.at[slot], merge_all.at[t])

            loop(1, G, to_group)
            loop(1, n, to_all)
            loop(0, groups, to_owners)
            wire.keep(0, one.at[m], one_all.at[m])
            attend_to(me, wire.keep)
            wire.keep(3, vec.at[me], vec_all.at[me])
            wire.kept(0, one_all.at[0])
            wire.kept(1, attend.at[0])
            wire.kept(3, vec_all.at[0])
            wire.settle(0, one_all.at[pl.ds(0, G - 1)])
            wire.settle(1, attend.at[pl.ds(0, n - 1)])
            wire.settle(3, vec_all.at[pl.ds(0, n - 1)])

            @pl.when(me // groups == m)
            def _():
                wire.kept(2, merge_all.at[0])
                wire.settle(2, merge_all.at[pl.ds(0, groups - 1)])

            @pl.when(me // groups != m)
            def _():
                wire.settle(2, merge_all)

        one_parts, attend_parts, merge_parts, vec_parts = exchange(
            scatter_first,
            "scatter_first",
            7,
            n,
            fsdp,
            4,
            (
                grad_one_part.astype(BF16).reshape(G, rows, width),
                grad_attend_part.reshape(n, depth, 3 * slice_width),
                grad_merge_part.reshape(groups, depth, width),
                packed_grads,
            ),
            (
                ((G, rows, width), BF16),
                ((groups, depth, 3 * width), BF16),
                ((groups, depth, width), BF16),
                ((n, vec_rows, 128), F32),
            ),
        )
        grad_one = jnp.sum(one_parts.astype(F32), axis=0)
        scaled_one, inverse_one = normalize(block_in)
        input_grad = grad_hidden + normalize_back(grad_one, scaled_one, inverse_one, gain_one)
        grad_attend_weight = jnp.sum(attend_parts.astype(F32), axis=0)
        grad_merge_weight = jnp.sum(merge_parts.astype(F32), axis=0)
        vec_sums = jnp.sum(vec_parts, axis=0).reshape(-1)
        (g_gain_one, g_shift_one, g_attend_bias, g_merge_bias, g_gain_two, g_shift_two, g_expand_bias, g_shrink_bias) = (
            vec_sums[spot : spot + size] for spot, size in zip(spots, sizes)
        )
        return (
            residual_out,
            input_grad,
            g_gain_one,
            g_shift_one,
            grad_attend_weight,
            g_attend_bias,
            grad_merge_weight,
            g_merge_bias,
            g_gain_two,
            g_shift_two,
            grad_expand_weight,
            g_expand_bias,
            grad_shrink_weight,
            g_shrink_bias,
        )

    return on_device


def solution(mesh):
    rows, line = P(("ctx", "fsdp"), None), P(("ctx", "fsdp"))
    n, fsdp = mesh.shape["ctx"] * mesh.shape["fsdp"], mesh.shape["fsdp"]
    return jax.shard_map(
        layer(n, fsdp),
        mesh=mesh,
        in_specs=(rows, line, line, rows, line, rows, line, line, line, rows, line, rows, line, rows),
        out_specs=(rows, rows, line, line, rows, line, rows, line, line, line, rows, line, rows, line),
        check_vma=False,
    )
```

```python
import math

import jax
import jax.numpy as jnp
from jax import lax
from jax.experimental import pallas as pl
from jax.experimental.pallas import tpu as pltpu
from jax.sharding import PartitionSpec as P

H = 16
G = 8
UNITS = 128
EPSILON = 1e-05
GELU_SCALE = 0.7978845608028654
GELU_CUBIC = 0.044715
LOG2E = 1.4426950408889634
MESH = pl.DeviceIdType.MESH
BF16 = jnp.bfloat16
F32 = jnp.float32
VMEM = pl.BlockSpec(memory_space=pltpu.VMEM)
ANY = pl.BlockSpec(memory_space=pl.ANY)


def position(fsdp):
    return lax.axis_index("ctx") * fsdp + lax.axis_index("fsdp")


def flip(number, bit):
    return number + bit - 2 * bit * lax.rem(number // bit, 2)


def span(index, size):
    return pl.ds(pl.multiple_of(index * size, size), size)


def loop(low, high, step):
    def turn(index, carry):
        step(index)
        return carry

    lax.fori_loop(low, high, turn, 0)


def dot(left, right, left_dim, right_dim):
    return lax.dot_general(
        left, right, (((left_dim,), (right_dim,)), ((), ())), preferred_element_type=F32
    )


class Sizes:
    def __init__(self, n, fsdp):
        self.n, self.fsdp = n, fsdp
        self.groups = n // G
        self.parts = self.groups // 2
        self.chips = self.groups // 4
        self.per_group = G // self.parts


class Wire:
    def __init__(self, sizes, send, recv, local):
        self.sizes = sizes
        self.n, self.fsdp = sizes.n, sizes.fsdp
        self.send, self.recv, self.local = send, recv, local
        self.me = position(self.fsdp)
        self.t, self.m = self.me // G, lax.rem(self.me, G)
        self.core = lax.rem(self.m // 2, 2)
        self.sibling = flip(self.me, 2)
        self.peers = [flip(self.m, 1), flip(self.m, 4), flip(flip(self.m, 1), 4)]
        self.quarter = self.t // sizes.chips
        self.part = lax.rem(self.t, sizes.chips) * 2 + self.core
        self.source_core = self.quarter // 2
        self.source_m = self.m + 2 * (self.source_core - self.core)
        self.which = lax.rem(self.quarter, 2)
        self.head = 2 * self.source_m + self.which

    def where(self, device):
        return (device // self.fsdp, lax.rem(device, self.fsdp))

    def greet(self):
        barrier = pltpu.get_barrier_semaphore()

        def hello(step):
            other = lax.rem(self.me + step, self.n)
            pl.semaphore_signal(barrier, inc=1, device_id=self.where(other), device_id_type=MESH)

        loop(1, self.n, hello)
        pl.semaphore_wait(barrier, self.n - 1)

    def put(self, lane, source, target, device):
        pltpu.make_async_remote_copy(
            src_ref=source,
            dst_ref=target,
            send_sem=self.send.at[lane],
            recv_sem=self.recv.at[lane],
            device_id=self.where(device),
            device_id_type=MESH,
        ).start()

    def keep(self, lane, source, target):
        pltpu.make_async_copy(source, target, self.local.at[lane]).start()

    def give(self, lane, source, target, device):
        @pl.when(device != self.me)
        def _():
            self.put(lane, source, target, device)

        @pl.when(device == self.me)
        def _():
            self.keep(lane, source, target)

    def kept(self, lane, like):
        pltpu.make_async_copy(like, like, self.local.at[lane]).wait()

    def sent(self, lane, like):
        pltpu.make_async_copy(like, like, self.send.at[lane]).wait()

    def came(self, lane, like):
        pltpu.make_async_copy(like, like, self.recv.at[lane]).wait()

    def settle(self, lane, like):
        self.came(lane, like)
        self.sent(lane, like)

    def settle_given(self, lane, mine, less, whole):
        @pl.when(mine)
        def _():
            self.kept(lane, whole[0])
            self.settle(lane, less)

        @pl.when(jnp.logical_not(mine))
        def _():
            self.settle(lane, whole[1])

    def group(self, step):
        m = lax.rem(self.m + step, G)
        return m, self.t * G + m

    def column(self, step):
        t = lax.rem(self.t + step, self.sizes.groups)
        return t, t * G + self.m


class Gather:
    LANES = 4

    def __init__(self, wire, lane, block, place, four):
        self.wire, self.lane, self.block, self.place, self.four = wire, lane, block, place, four

    def start(self):
        wire, mine = self.wire, self.place(self.wire.m)
        for k, m in enumerate(wire.peers):
            wire.put(self.lane + k, self.block, mine, wire.t * G + m)
        wire.put(self.lane + 3, self.block, mine, wire.sibling)
        wire.keep(self.lane, self.block, mine)

    def forward(self):
        wire = self.wire
        for k, m in enumerate(wire.peers):
            wire.came(self.lane + k, self.place(m))
            wire.put(self.lane + 3, self.place(m), self.place(m), wire.sibling)

    def finish(self):
        wire = self.wire
        wire.kept(self.lane, self.place(wire.m))
        for k in range(3):
            wire.sent(self.lane + k, self.place(wire.m))
        wire.settle(self.lane + 3, self.four)


class Scatter:
    LANES = 4

    def __init__(self, wire, lane, parts, got, summed, result):
        self.wire, self.lane = wire, lane
        self.parts, self.got, self.summed, self.result = parts, got, summed, result

    def start(self):
        wire = self.wire
        for k, m in enumerate([wire.m] + wire.peers):
            wire.put(self.lane + 3, self.parts.at[flip(m, 2)], self.got.at[k], wire.sibling)

    def forward(self):
        wire = self.wire
        wire.came(self.lane + 3, self.got)
        rows = self.got.shape[1]
        step = 16
        for k, m in reversed(list(enumerate([wire.m] + wire.peers))):

            def add(i, k=k, m=m):
                at = span(i, step)
                total = self.parts[m, at, :].astype(F32) + self.got[k, at, :].astype(F32)
                self.summed[k, at, :] = total.astype(BF16)

            loop(0, rows // step, add)
            if k:
                wire.put(self.lane + k - 1, self.summed.at[k], self.result.at[k], wire.t * G + m)
            else:
                wire.keep(self.lane, self.summed.at[0], self.result.at[0])

    def finish(self):
        wire = self.wire
        wire.sent(self.lane + 3, self.got)
        wire.kept(self.lane, self.result.at[0])
        for k in range(3):
            wire.settle(self.lane + k, self.result.at[k + 1])


def scatter_scratch(rows, width):
    return [pltpu.VMEM((4, rows, width), BF16), pltpu.VMEM((4, rows, width), BF16)]


def exchange(body, name, number, sizes, lanes, inputs, outs, scratch=(), vmem_outs=0):
    def kernel(*refs):
        ins = refs[: len(inputs)]
        results = refs[len(inputs) : len(inputs) + len(outs)]
        extra = refs[len(inputs) + len(outs) : len(refs) - 3]
        wire = Wire(sizes, *refs[len(refs) - 3 :])
        wire.greet()
        body(wire, *ins, *results, *extra)

    kernel.__name__ = name
    return pl.pallas_call(
        kernel,
        out_shape=[jax.ShapeDtypeStruct(shape, kind) for shape, kind in outs],
        in_specs=[VMEM] * len(inputs),
        out_specs=[VMEM] * vmem_outs + [ANY] * (len(outs) - vmem_outs),
        scratch_shapes=[*scratch, *([pltpu.SemaphoreType.DMA((lanes,))] * 3)],
        compiler_params=pltpu.CompilerParams(collective_id=number, has_side_effects=True),
        name=name,
    )(*inputs)


def normalize(inputs):
    centred = inputs - jnp.mean(inputs, axis=1, keepdims=True)
    inverse = lax.rsqrt(jnp.mean(centred * centred, axis=1, keepdims=True) + EPSILON)
    return centred * inverse, inverse


def normalize_back(grad_norm, scaled, inverse, gain_row):
    grad_scaled = grad_norm * gain_row
    mean_one = jnp.mean(grad_scaled, axis=1, keepdims=True)
    mean_two = jnp.mean(grad_scaled * scaled, axis=1, keepdims=True)
    return inverse * (grad_scaled - mean_one - scaled * mean_two)


def gelu_pair(pre_act):
    tangent = jnp.tanh(GELU_SCALE * (pre_act + GELU_CUBIC * pre_act * pre_act * pre_act))
    activated = 0.5 * pre_act * (1.0 + tangent)
    derivative = 0.5 * (1.0 + tangent) + 0.5 * pre_act * (1.0 - tangent * tangent) * GELU_SCALE * (
        1.0 + 3.0 * GELU_CUBIC * pre_act * pre_act
    )
    return (activated, derivative)


def tiles_of(queries, parts):
    wide = min(256, queries)
    deep = min(512, wide * parts)
    return wide, deep, wide * parts // deep


def query_places(tile, wide, parts, part):
    column = lax.broadcasted_iota(jnp.int32, (1, wide), 1)
    block = tile * (wide // 128) + column // 128
    return (block * parts + part) * 128 + lax.rem(column, 128)


def attend_tiles(wire, query_ref, pair_ref, out_ref, total_ref, key_ref, after):
    width, queries = query_ref.shape
    keys = pair_ref.shape[2]
    parts = wire.sizes.parts
    wide, deep, band = tiles_of(queries, parts)
    factor = LOG2E / math.sqrt(width)

    def turn(j):
        at = span(j, deep)
        key_ref[at, :] = pair_ref[0, :, at].T

    loop(0, keys // deep, turn)

    def tile_step(tile):
        mine = span(tile, wide)
        query = query_ref[:, mine]
        places = query_places(tile, wide, parts, wire.part)

        def step(j, carry, masked):
            best, total, summed = carry
            at = span(j, deep)
            scores = dot(key_ref[at, :], query, 1, 0)
            if masked:
                key_places = j * deep + lax.broadcasted_iota(jnp.int32, (deep, wide), 0)
                scores = jnp.where(key_places <= places, scores, -1e30)
            higher = jnp.maximum(best, jnp.max(scores, axis=0, keepdims=True))
            weights = jnp.exp2((scores - higher) * factor)
            shrunk = jnp.exp2((best - higher) * factor)
            total = total * shrunk + jnp.sum(weights, axis=0, keepdims=True)
            summed = summed * shrunk + dot(pair_ref[1, :, at], weights.astype(BF16), 1, 0)
            return higher, total, summed

        carry = (
            jnp.full((1, wide), -1e30, F32),
            jnp.zeros((1, wide), F32),
            jnp.zeros((width, wide), F32),
        )
        carry = lax.fori_loop(0, tile * band, lambda j, c: step(j, c, False), carry)
        for extra in range(band):
            carry = step(tile * band + extra, carry, True)
        best, total, summed = carry
        out_ref[:, mine] = (summed / total).astype(BF16)
        total_ref[:, mine] = best * factor + jnp.log2(total)
        after(tile)

    loop(0, queries // wide, tile_step)


def attend_back_tiles(
    wire, query_ref, pair_ref, grad_ref, out_ref, total_ref, dq_ref, dpair_ref, query_rows, grad_rows, delta_ref, dq_sum, after
):
    width, queries = query_ref.shape
    keys = pair_ref.shape[2]
    parts = wire.sizes.parts
    wide, deep, band = tiles_of(queries, parts)
    scale = 1.0 / math.sqrt(width)
    factor = LOG2E * scale

    def prepare(tile):
        mine = span(tile, wide)
        grad = grad_ref[:, mine]
        query_rows[mine, :] = query_ref[:, mine].T
        grad_rows[mine, :] = grad.T
        delta_ref[:, mine] = jnp.sum(grad.astype(F32) * out_ref[:, mine].astype(F32), axis=0, keepdims=True)
        dq_sum[:, mine] = jnp.zeros((width, wide), F32)

    loop(0, queries // wide, prepare)

    def key_step(j):
        at = span(j, deep)
        key_t, value_t = pair_ref[0, :, at], pair_ref[1, :, at]
        key, value = key_t.T, value_t.T
        key_places = j * deep + lax.broadcasted_iota(jnp.int32, (deep, wide), 0)

        def step(tile, carry, masked):
            dkey, dvalue = carry
            mine = span(tile, wide)
            scores = dot(key, query_ref[:, mine], 1, 0) * factor
            if masked:
                places = query_places(tile, wide, parts, wire.part)
                scores = jnp.where(key_places <= places, scores, -1e30)
            probs = jnp.exp2(scores - total_ref[:, mine])
            dvalue = dvalue + dot(probs.astype(BF16), grad_rows[mine, :], 1, 0)
            grad_probs = dot(value, grad_ref[:, mine], 1, 0)
            grad_scores = (probs * (grad_probs - delta_ref[:, mine]) * scale).astype(BF16)
            dkey = dkey + dot(grad_scores, query_rows[mine, :], 1, 0)
            dq_sum[:, mine] += dot(key_t, grad_scores, 1, 0)
            return dkey, dvalue

        first = j // band
        carry = (jnp.zeros((deep, width), F32), jnp.zeros((deep, width), F32))
        carry = step(first, carry, True)
        dkey, dvalue = lax.fori_loop(first + 1, queries // wide, lambda i, c: step(i, c, False), carry)
        dpair_ref[0, :, at] = dkey.T.astype(BF16)
        dpair_ref[1, :, at] = dvalue.T.astype(BF16)

        @pl.when(lax.rem(j, band) == band - 1)
        def _():
            mine = span(first, wide)
            dq_ref[:, mine] = dq_sum[:, mine].astype(BF16)

        after(j, first, lax.rem(j, band) == band - 1)

    loop(0, keys // deep, key_step)


def layer(n, fsdp):
    sizes = Sizes(n, fsdp)
    groups, parts, per_group = sizes.groups, sizes.parts, sizes.per_group

    def on_device(
        residual_in,
        first_gain,
        first_shift,
        attend_weight,
        attend_bias,
        merge_weight,
        merge_bias,
        second_gain,
        second_shift,
        expand_weight,
        expand_bias,
        shrink_weight,
        shrink_bias,
        cotangent,
    ):
        rows, width = residual_in.shape
        depth = width // n
        hidden_rows = shrink_weight.shape[0]
        hidden_units = expand_weight.shape[1]
        slice_width = width // G
        slice_units = hidden_units // G
        blocks = slice_units // UNITS
        shares = UNITS // hidden_rows
        head = width // H
        group_rows = rows * G
        half = group_rows // 2
        tokens = rows * n
        queries = tokens // parts
        chunk = per_group * rows
        me = position(fsdp)
        member = lax.rem(me, G)

        small = (first_gain, first_shift, attend_bias, merge_bias, second_gain, second_shift, expand_bias, shrink_bias)
        counts = [s.shape[0] for s in small]
        packed_rows = -(-sum(counts) // 2048) * 16
        packed = jnp.pad(jnp.concatenate(small), (0, packed_rows * 128 - sum(counts))).reshape(packed_rows, 128)

        def unit_block(q, m):
            return span(q * G + m, UNITS)

        def gather_first(wire, x, attend, merge, vec, expand, x_all, attend_all, merge_all, vec_all, expand_all):
            me, t, m = wire.me, wire.t, wire.m
            x_gather = Gather(wire, 4, x, lambda k: x_all.at[k], x_all.at[pl.ds(0, 4)])
            x_gather.start()

            def attend_to(other, move):
                for p in range(3):
                    columns = pl.ds(pl.multiple_of(p * width + other * slice_width, 128), slice_width)
                    move(0, attend.at[:, columns], attend_all.at[me, :, pl.ds(p * slice_width, slice_width)])

            def to_all(step):
                device = lax.rem(me + step, n)
                attend_to(lax.rem(device, G), lambda lane, s, d: wire.put(lane, s, d, device))
                wire.put(1, vec, vec_all.at[me], device)

            def expand_to(other, move):
                for q in range(blocks):
                    move(3, expand.at[:, unit_block(q, other)], expand_all.at[m, :, pl.ds(q * UNITS, UNITS)])

            def to_group(step):
                other, device = wire.group(step)
                expand_to(other, lambda lane, s, d: wire.put(lane, s, d, device))

            def to_column(step):
                _, device = wire.column(step)
                wire.put(2, merge, merge_all.at[t], device)

            loop(1, n, to_all)
            loop(1, groups, to_column)
            loop(1, G, to_group)
            attend_to(m, wire.keep)
            wire.keep(1, vec, vec_all.at[me])
            wire.keep(2, merge, merge_all.at[t])
            expand_to(m, wire.keep)
            wire.kept(0, attend_all.at[0])
            wire.kept(1, vec_all.at[0])
            wire.kept(2, merge_all.at[0])
            wire.kept(3, expand_all.at[0])
            x_gather.forward()
            wire.settle(0, attend_all.at[pl.ds(0, n - 1)])
            wire.settle(1, vec_all.at[pl.ds(0, n - 1)])
            wire.settle(2, merge_all.at[pl.ds(0, groups - 1)])
            wire.settle(3, expand_all.at[pl.ds(0, G - 1)])
            x_gather.finish()

        x_all, attend_all, merge_all, vec_all, expand_group = exchange(
            gather_first,
            "gather_first",
            0,
            sizes,
            8,
            (residual_in, attend_weight, merge_weight, packed, expand_weight),
            (
                ((G, rows, width), BF16),
                ((n, depth, 3 * slice_width), BF16),
                ((groups, depth, width), BF16),
                ((n, packed_rows, 128), BF16),
                ((G, depth, slice_units), BF16),
            ),
        )
        flat = vec_all.reshape(n, packed_rows * 128)
        spots = [sum(counts[:k]) for k in range(len(counts))]
        gain_one, shift_one, attend_shift, merge_shift, gain_two, shift_two, expand_shift, shrink_shift = (
            flat[:, spot : spot + count].reshape(-1).astype(F32) for spot, count in zip(spots, counts)
        )
        attend_slice = attend_all.reshape(width, 3 * slice_width)

        scaled_group, _ = normalize(x_all.reshape(group_rows, width).astype(F32))
        input_one = (scaled_group * gain_one + shift_one).astype(BF16)
        bias_mine = jnp.concatenate(
            [
                lax.dynamic_slice_in_dim(attend_shift, member * slice_width, slice_width),
                jnp.zeros((slice_width,), F32),
                lax.dynamic_slice_in_dim(attend_shift, width + member * slice_width, slice_width),
            ]
        )
        projected = (dot(attend_slice, input_one, 0, 1) + bias_mine[:, None]).astype(BF16)
        projected = projected.reshape(3, 2, head, group_rows)

        def spread_heads(wire, qkv, merge, pair, query, merge_full):
            t, m, core = wire.t, wire.m, wire.core
            chips = sizes.chips
            own = core == wire.source_core
            merge_gather = Gather(wire, 3, merge, lambda k: merge_full.at[:, k], merge_full.at[:, pl.ds(0, 4)])
            first = 7

            def to_chip(step):
                other = lax.rem(core * 2 * chips + lax.rem(t + step, 2 * chips), groups)
                which = lax.rem(other // chips, 2)
                for c in range(2):
                    device = other * G + m + 2 * (c - core)
                    mine = pl.ds(pl.multiple_of(t * group_rows + c * half, 128), half)
                    for kind in range(2):
                        wire.give(first + t, qkv.at[1 + kind, which, :, pl.ds(c * half, half)], pair.at[kind, :, mine], device)

            def queries_to(step):
                other = lax.rem(core * 2 * chips + lax.rem(t + step, 2 * chips), groups)
                which = lax.rem(other // chips, 2)
                for c in range(2):
                    device = other * G + m + 2 * (c - core)
                    part = lax.rem(other, chips) * 2 + c
                    for i in range(per_group):
                        source = span(part + i * parts, rows)
                        target = span(t * per_group + i, rows)
                        wire.give(0, qkv.at[0, which, :, source], query.at[:, target], device)

            loop(0, 2 * chips, to_chip)
            loop(0, 2 * chips, queries_to)
            merge_gather.start()

            def pass_on(step):
                other = lax.rem(t + step, groups)
                piece = pair.at[:, :, pl.ds(pl.multiple_of(other * group_rows + core * half, 128), half)]
                here = jnp.logical_and(own, other == t)

                @pl.when(here)
                def _():
                    wire.kept(first + other, piece)

                @pl.when(jnp.logical_not(here))
                def _():
                    wire.came(first + other, piece)

                wire.put(1, piece, piece, wire.sibling)

            loop(0, groups, pass_on)
            merge_gather.forward()
            all_halves = pair.at[:, :, pl.ds(0, tokens // 2)]
            wire.settle(1, all_halves)
            merge_gather.finish()

            @pl.when(own)
            def _():
                wire.sent(first + t, pair.at[:, :, pl.ds(0, (groups - 1) * half)])
                wire.kept(0, query.at[:, pl.ds(0, chunk)])
                wire.settle(0, query.at[:, pl.ds(0, queries - chunk)])

            @pl.when(jnp.logical_not(own))
            def _():
                wire.sent(first + t, all_halves)
                wire.settle(0, query)

        pair_t, query_t, merge_full = exchange(
            spread_heads,
            "spread_heads",
            1,
            sizes,
            7 + groups,
            (projected, merge_all),
            (((2, head, tokens), BF16), ((head, queries), BF16), ((groups, G, depth, width), BF16)),
        )
        merge_full = merge_full.reshape(width, width)

        def attend(wire, query, pair, expand, cot, out, total, attended, expand_all, cot_all, keys_scratch):
            me, t = wire.me, wire.t
            cot_gather = Gather(wire, 2, cot, lambda k: cot_all.at[k], cot_all.at[pl.ds(0, 4)])

            def to_column(step):
                _, device = wire.column(step)
                wire.put(1, expand, expand_all.at[t], device)

            loop(1, groups, to_column)
            cot_gather.start()
            wire.keep(1, expand, expand_all.at[t])
            place = span(wire.head, head)
            wide = tiles_of(queries, parts)[0]

            def after(tile):
                for b in range(wide // rows):
                    block = tile * (wide // rows) + b
                    wire.give(0, out.at[:, span(block, rows)], attended.at[place, :], block * parts + wire.part)

                @pl.when(tile == queries // wide - 2)
                def _():
                    cot_gather.forward()

            attend_tiles(wire, query, pair, out, total, keys_scratch, after)
            mine = lax.rem(me, parts) == wire.part

            @pl.when(mine)
            def _():
                wire.kept(0, attended.at[pl.ds(0, head), :])
                wire.came(0, attended.at[pl.ds(0, width - head), :])
                wire.sent(0, out.at[:, pl.ds(0, queries - rows)])

            @pl.when(jnp.logical_not(mine))
            def _():
                wire.came(0, attended)
                wire.sent(0, out)

            wire.kept(1, expand_all.at[0])
            wire.settle(1, expand_all.at[pl.ds(0, groups - 1)])
            cot_gather.finish()

        out_t, log_total, attended_t, expand_all, cot_all = exchange(
            attend,
            "attend",
            2,
            sizes,
            6,
            (query_t, pair_t, expand_group, cotangent),
            (
                ((head, queries), BF16),
                ((1, queries), F32),
                ((width, rows), BF16),
                ((groups, G, depth, slice_units), BF16),
                ((G, rows, width), BF16),
            ),
            scratch=[pltpu.VMEM((tokens, head), BF16)],
            vmem_outs=2,
        )

        block_in = residual_in.astype(F32)
        hidden = block_in + (dot(attended_t, merge_full, 0, 0) + merge_shift)
        scaled_two, inverse_two = normalize(hidden)
        input_two = (scaled_two * gain_two + shift_two).astype(BF16)

        def gather_second(wire, normed, shrink, normed_all, shrink_all):
            me, t = wire.me, wire.t
            block = me // shares
            user = lax.rem(block, G)
            normed_gather = Gather(wire, 1, normed, lambda k: normed_all.at[k], normed_all.at[pl.ds(0, 4)])
            normed_gather.start()

            def to_users(step):
                other = lax.rem(t + step, groups)
                wire.give(0, shrink, shrink_all.at[block // G * shares + lax.rem(me, shares)], other * G + user)

            loop(0, groups, to_users)
            normed_gather.forward()
            wire.settle_given(0, user == wire.m, shrink_all.at[pl.ds(0, groups - 1)], (shrink, shrink_all))
            normed_gather.finish()

        normed_all, shrink_all = exchange(
            gather_second,
            "gather_second",
            3,
            sizes,
            5,
            (input_two, shrink_weight),
            (((G, rows, width), BF16), ((groups, hidden_rows, width), BF16)),
        )
        group_two = normed_all.reshape(group_rows, width)
        group_cot = cot_all.reshape(group_rows, width)
        expand_slice = expand_all.reshape(width, slice_units)
        shrink_slice = shrink_all.reshape(slice_units, width)
        shift_units = lax.dynamic_index_in_dim(expand_shift.reshape(blocks, G, UNITS), member, 1, False).reshape(-1)
        activated, derivative = gelu_pair(dot(group_two, expand_slice, 1, 0) + shift_units)
        act_input = activated.astype(BF16)
        shrunk_part = dot(act_input, shrink_slice, 1, 0).astype(BF16)
        grad_shrink_part = dot(act_input, group_cot, 0, 0).astype(BF16)
        grad_pre = dot(group_cot, shrink_slice, 1, 1) * derivative
        grad_expand_shift = jnp.sum(grad_pre, axis=0)
        grad_pre_input = grad_pre.astype(BF16)
        grad_expand_part = dot(group_two, grad_pre_input, 0, 0).astype(BF16)
        grad_two_part = dot(grad_pre_input, expand_slice, 1, 1).astype(BF16)

        def scatter_second(wire, two, shrink, two_all, shrink_all, got, summed):
            me, t, m = wire.me, wire.t, wire.m
            two_scatter = Scatter(wire, 1, two, got, summed, two_all)
            two_scatter.start()

            def to_owners(step):
                piece = lax.rem(step + t, groups)
                owner = (piece // shares * G + m) * shares + lax.rem(piece, shares)
                wire.give(0, shrink.at[piece], shrink_all.at[t], owner)

            loop(0, groups, to_owners)
            two_scatter.forward()
            wire.settle_given(
                0, lax.rem(me // shares, G) == m, shrink_all.at[pl.ds(0, groups - 1)], (shrink_all.at[0], shrink_all)
            )
            two_scatter.finish()

        two_parts, shrink_parts = exchange(
            scatter_second,
            "scatter_second",
            4,
            sizes,
            5,
            (
                grad_two_part.reshape(G, rows, width),
                grad_shrink_part.reshape(groups, hidden_rows, width),
            ),
            (((4, rows, width), BF16), ((groups, hidden_rows, width), BF16)),
            scratch=scatter_scratch(rows, width),
        )
        grad_shrink_weight = jnp.sum(shrink_parts.astype(F32), axis=0)
        grad_top = cotangent.astype(F32)
        grad_shrink_shift = jnp.sum(grad_top, axis=0)
        grad_two = jnp.sum(two_parts.astype(F32), axis=0)
        grad_gain_two = jnp.sum(grad_two * scaled_two, axis=0)
        grad_shift_two = jnp.sum(grad_two, axis=0)
        grad_hidden = grad_top + normalize_back(grad_two, scaled_two, inverse_two, gain_two)
        grad_merge_shift = jnp.sum(grad_hidden, axis=0)
        grad_hidden_input = grad_hidden.astype(BF16)
        grad_attended_t = dot(merge_full, grad_hidden_input, 1, 1).astype(BF16)

        def send_grad(wire, grad, grad_out):
            me = wire.me
            part = lax.rem(me, parts)
            place = span(me // parts, rows)

            def to_head(step):
                h = lax.rem(step + me, H)
                source_m = h // 2
                quarter = lax.rem(source_m // 2, 2) * 2 + lax.rem(h, 2)
                t = quarter * sizes.chips + part // 2
                device = t * G + source_m + 2 * (lax.rem(part, 2) - lax.rem(source_m // 2, 2))
                wire.give(0, grad.at[span(h, head), :], grad_out.at[:, place], device)

            loop(0, H, to_head)
            mine = wire.part == part

            @pl.when(mine)
            def _():
                wire.kept(0, grad.at[pl.ds(0, head), :])
                wire.came(0, grad_out.at[:, pl.ds(0, queries - rows)])
                wire.sent(0, grad.at[pl.ds(0, width - head), :])

            @pl.when(jnp.logical_not(mine))
            def _():
                wire.came(0, grad_out)
                wire.sent(0, grad)

        (grad_t,) = exchange(send_grad, "send_grad", 5, sizes, 1, (grad_attended_t,), (((head, queries), BF16),))

        def attend_back(
            wire, query, pair, grad, out, total, shrunk, hidden_grad, att, expand,
            dq, dpair, dq_all, dpair_all, shrunk_all, hidden_all, att_all, expand_all,
            query_rows, grad_rows, delta, dq_sum, got, summed,
        ):
            me, t, m = wire.me, wire.t, wire.m
            shrunk_scatter = Scatter(wire, 4, shrunk, got, summed, shrunk_all)
            hidden_gather = Gather(wire, 8, hidden_grad, lambda k: hidden_all.at[k], hidden_all.at[pl.ds(0, 4)])
            shrunk_scatter.start()
            hidden_gather.start()
            place = pl.ds(pl.multiple_of(m * rows, 128), rows)

            def to_group(step):
                other, device = wire.group(step)
                wire.put(2, att.at[span(other, slice_width), :], att_all.at[:, place], device)

            loop(1, G, to_group)
            wire.keep(2, att.at[span(m, slice_width), :], att_all.at[:, place])
            shrunk_scatter.forward()
            wide, deep, band = tiles_of(queries, parts)

            def after(j, first, final):
                place_in_group = pl.ds(pl.multiple_of(lax.rem(j * deep, group_rows), deep), deep)
                device = j * deep // group_rows * G + wire.source_m
                wire.give(0, dpair.at[:, :, span(j, deep)], dpair_all.at[wire.part, wire.which, :, :, place_in_group], device)

                @pl.when(final)
                def _():
                    for b in range(wide // rows):
                        block = first * (wide // rows) + b
                        owner = block * parts + wire.part
                        wire.give(
                            1,
                            dq.at[:, span(block, rows)],
                            dq_all.at[wire.which, :, span(lax.rem(owner, G), rows)],
                            owner // G * G + wire.source_m,
                        )

                @pl.when(j == 2)
                def _():
                    def to_column(step):
                        other, device = wire.column(step)
                        wire.put(3, expand.at[other], expand_all.at[t], device)

                    loop(1, groups, to_column)
                    wire.keep(3, expand.at[t], expand_all.at[t])

                @pl.when(j == keys_tiles - 2)
                def _():
                    hidden_gather.forward()

            keys_tiles = tokens // deep
            attend_back_tiles(
                wire, query, pair, grad, out, total, dq, dpair, query_rows, grad_rows, delta, dq_sum, after
            )
            own = wire.core == wire.source_core

            @pl.when(own)
            def _():
                wire.kept(0, dpair.at[:, :, pl.ds(0, group_rows)])
                wire.kept(1, dq.at[:, pl.ds(0, chunk)])
                wire.sent(0, dpair.at[:, :, pl.ds(0, tokens - group_rows)])
                wire.sent(1, dq.at[:, pl.ds(0, queries - chunk)])
                wire.came(0, dpair.at[:, :, pl.ds(0, tokens - group_rows)])
                wire.came(1, dq.at[:, pl.ds(0, queries - chunk)])

            @pl.when(jnp.logical_not(own))
            def _():
                wire.sent(0, dpair)
                wire.sent(1, dq)
                wire.came(0, dpair)
                wire.came(1, dq)

            wire.kept(2, att_all.at[:, pl.ds(0, rows)])
            wire.settle(2, att_all.at[:, pl.ds(0, group_rows - rows)])
            wire.kept(3, expand_all.at[0])
            wire.settle(3, expand_all.at[pl.ds(0, groups - 1)])
            shrunk_scatter.finish()
            hidden_gather.finish()

        _, _, dq_all, dpair_all, shrunk_parts, grad_all, att_all, expand_parts = exchange(
            attend_back,
            "attend_back",
            6,
            sizes,
            12,
            (
                query_t,
                pair_t,
                grad_t,
                out_t,
                log_total,
                shrunk_part.reshape(G, rows, width),
                grad_hidden_input,
                attended_t,
                grad_expand_part.reshape(groups, G * depth, slice_units),
            ),
            (
                ((head, queries), BF16),
                ((2, head, tokens), BF16),
                ((2, head, group_rows), BF16),
                ((parts, 2, 2, head, group_rows), BF16),
                ((4, rows, width), BF16),
                ((G, rows, width), BF16),
                ((slice_width, group_rows), BF16),
                ((groups, G * depth, slice_units), BF16),
            ),
            scratch=[
                pltpu.VMEM((queries, head), BF16),
                pltpu.VMEM((queries, head), BF16),
                pltpu.VMEM((1, queries), F32),
                pltpu.VMEM((head, queries), F32),
                *scatter_scratch(rows, width),
            ],
            vmem_outs=2,
        )
        residual_out = (hidden + jnp.sum(shrunk_parts.astype(F32), axis=0) + shrink_shift).astype(BF16)
        grad_expand_group = jnp.sum(expand_parts.astype(F32), axis=0).astype(BF16).reshape(G, depth, slice_units)
        grad_pair = jnp.sum(dpair_all.astype(F32), axis=0)
        grad_projected = jnp.concatenate(
            [
                dq_all.astype(F32).reshape(slice_width, group_rows),
                grad_pair[:, 0].reshape(slice_width, group_rows),
                grad_pair[:, 1].reshape(slice_width, group_rows),
            ],
            axis=0,
        )
        grad_shift_mine = jnp.sum(grad_projected, axis=1)
        grad_projected = grad_projected.astype(BF16)
        grad_attend_part = dot(input_one, grad_projected, 0, 1).astype(BF16)
        grad_one_part = dot(grad_projected, attend_slice, 0, 1)
        grad_gain_one = jnp.sum(grad_one_part * scaled_group, axis=0)
        grad_shift_one = jnp.sum(grad_one_part, axis=0)
        grad_merge_part = dot(att_all, grad_all.reshape(group_rows, width), 1, 0).astype(BF16)

        grad_attend_shift = jnp.zeros((2 * width,), F32)
        grad_attend_shift = lax.dynamic_update_slice_in_dim(
            grad_attend_shift, grad_shift_mine[:slice_width], member * slice_width, 0
        )
        grad_attend_shift = lax.dynamic_update_slice_in_dim(
            grad_attend_shift, grad_shift_mine[2 * slice_width :], width + member * slice_width, 0
        )
        grad_expand_all = lax.dynamic_update_slice_in_dim(
            jnp.zeros((blocks, G, UNITS), F32), grad_expand_shift.reshape(blocks, 1, UNITS), member, 1
        ).reshape(-1)
        grads = (
            grad_gain_one,
            grad_shift_one,
            grad_attend_shift,
            grad_merge_shift,
            grad_gain_two,
            grad_shift_two,
            grad_expand_all,
            grad_shrink_shift,
        )
        total_size = sum(counts)
        vec_rows = -(-total_size // 1024) * 8
        packed_grads = jnp.pad(
            jnp.concatenate([g.reshape(n, -1) for g in grads], axis=1), ((0, 0), (0, vec_rows * 128 - total_size))
        ).reshape(n, vec_rows, 128)

        def scatter_first(wire, one, attend, merge, vec, expand, one_all, attend_all, merge_all, vec_all, expand_all, got, summed):
            me, t, m = wire.me, wire.t, wire.m
            one_scatter = Scatter(wire, 4, one, got, summed, one_all)
            one_scatter.start()

            def attend_to(device, move):
                for p in range(3):
                    columns = pl.ds(pl.multiple_of(p * width + m * slice_width, 128), slice_width)
                    move(1, attend.at[device, :, pl.ds(p * slice_width, slice_width)], attend_all.at[t, :, columns])

            def to_all(step):
                device = lax.rem(me + step, n)
                attend_to(device, lambda lane, s, d: wire.put(lane, s, d, device))
                wire.put(3, vec.at[device], vec_all.at[me], device)

            def to_owners(slot):
                wire.give(2, merge.at[slot], merge_all.at[t], m * groups + slot)

            def expand_to(other, move):
                for q in range(blocks):
                    move(0, expand.at[other, :, pl.ds(q * UNITS, UNITS)], expand_all.at[:, unit_block(q, m)])

            def to_group(step):
                other, device = wire.group(step)
                expand_to(other, lambda lane, s, d: wire.put(lane, s, d, device))

            loop(1, n // 2, to_all)
            one_scatter.forward()
            loop(n // 2, n, to_all)
            loop(0, groups, to_owners)
            loop(1, G, to_group)
            attend_to(me, wire.keep)
            expand_to(m, wire.keep)
            wire.keep(3, vec.at[me], vec_all.at[me])
            wire.kept(0, expand.at[0])
            wire.kept(1, attend.at[0])
            wire.kept(3, vec_all.at[0])
            wire.settle(0, expand.at[pl.ds(0, G - 1)])
            wire.settle(1, attend.at[pl.ds(0, n - 1)])
            wire.settle(3, vec_all.at[pl.ds(0, n - 1)])
            wire.settle_given(2, me // groups == m, merge_all.at[pl.ds(0, groups - 1)], (merge_all.at[0], merge_all))
            one_scatter.finish()

        one_parts, attend_parts, merge_parts, vec_parts, expand_whole = exchange(
            scatter_first,
            "scatter_first",
            7,
            sizes,
            8,
            (
                grad_one_part.astype(BF16).reshape(G, rows, width),
                grad_attend_part.reshape(n, depth, 3 * slice_width),
                grad_merge_part.reshape(groups, depth, width),
                packed_grads,
                grad_expand_group,
            ),
            (
                ((4, rows, width), BF16),
                ((groups, depth, 3 * width), BF16),
                ((groups, depth, width), BF16),
                ((n, vec_rows, 128), F32),
                ((depth, hidden_units), BF16),
            ),
            scratch=scatter_scratch(rows, width),
        )
        grad_one = jnp.sum(one_parts.astype(F32), axis=0)
        scaled_one, inverse_one = normalize(block_in)
        input_grad = grad_hidden + normalize_back(grad_one, scaled_one, inverse_one, gain_one)
        grad_attend_weight = jnp.sum(attend_parts.astype(F32), axis=0)
        grad_merge_weight = jnp.sum(merge_parts.astype(F32), axis=0)
        vec_sums = jnp.sum(vec_parts, axis=0).reshape(-1)
        (g_gain_one, g_shift_one, g_attend_bias, g_merge_bias, g_gain_two, g_shift_two, g_expand_bias, g_shrink_bias) = (
            vec_sums[spot : spot + count] for spot, count in zip(spots, counts)
        )
        return (
            residual_out,
            input_grad,
            g_gain_one,
            g_shift_one,
            grad_attend_weight,
            g_attend_bias,
            grad_merge_weight,
            g_merge_bias,
            g_gain_two,
            g_shift_two,
            expand_whole.astype(F32),
            g_expand_bias,
            grad_shrink_weight,
            g_shrink_bias,
        )

    return on_device


def solution(mesh):
    rows, line = P(("ctx", "fsdp"), None), P(("ctx", "fsdp"))
    n, fsdp = mesh.shape["ctx"] * mesh.shape["fsdp"], mesh.shape["fsdp"]
    return jax.shard_map(
        layer(n, fsdp),
        mesh=mesh,
        in_specs=(rows, line, line, rows, line, rows, line, line, line, rows, line, rows, line, rows),
        out_specs=(rows, rows, line, line, rows, line, rows, line, line, line, rows, line, rows, line),
        check_vma=False,
    )
```

```python
import math

import jax
import jax.numpy as jnp
from jax import lax
from jax.experimental import pallas as pl
from jax.experimental.pallas import tpu as pltpu
from jax.sharding import PartitionSpec as P

H = 16
G = 8
UNITS = 128
EPSILON = 1e-05
GELU_SCALE = 0.7978845608028654
GELU_CUBIC = 0.044715
LOG2E = 1.4426950408889634
MESH = pl.DeviceIdType.MESH
BF16 = jnp.bfloat16
F32 = jnp.float32
VMEM = pl.BlockSpec(memory_space=pltpu.VMEM)
ANY = pl.BlockSpec(memory_space=pl.ANY)


def position(fsdp):
    return lax.axis_index("ctx") * fsdp + lax.axis_index("fsdp")


def flip(number, bit):
    return number + bit - 2 * bit * lax.rem(number // bit, 2)


def span(index, size):
    return pl.ds(pl.multiple_of(index * size, size), size)


def loop(low, high, step):
    def turn(index, carry):
        step(index)
        return carry

    lax.fori_loop(low, high, turn, 0)


def dot(left, right, left_dim, right_dim):
    return lax.dot_general(
        left, right, (((left_dim,), (right_dim,)), ((), ())), preferred_element_type=F32
    )


class Sizes:
    def __init__(self, n, fsdp):
        self.n, self.fsdp = n, fsdp
        self.groups = n // G
        self.parts = self.groups // 2
        self.chips = self.groups // 4
        self.per_group = G // self.parts


class Wire:
    def __init__(self, sizes, send, recv, local):
        self.sizes = sizes
        self.n, self.fsdp = sizes.n, sizes.fsdp
        self.send, self.recv, self.local = send, recv, local
        self.me = position(self.fsdp)
        self.t, self.m = self.me // G, lax.rem(self.me, G)
        self.core = lax.rem(self.m // 2, 2)
        self.sibling = flip(self.me, 2)
        self.peers = [flip(self.m, 1), flip(self.m, 4), flip(flip(self.m, 1), 4)]
        self.quarter = self.t // sizes.chips
        self.part = lax.rem(self.t, sizes.chips) * 2 + self.core
        self.source_core = self.quarter // 2
        self.source_m = self.m + 2 * (self.source_core - self.core)
        self.which = lax.rem(self.quarter, 2)
        self.head = 2 * self.source_m + self.which

    def where(self, device):
        return (device // self.fsdp, lax.rem(device, self.fsdp))

    def greet(self):
        barrier = pltpu.get_barrier_semaphore()

        def hello(step):
            other = lax.rem(self.me + step, self.n)
            pl.semaphore_signal(barrier, inc=1, device_id=self.where(other), device_id_type=MESH)

        loop(1, self.n, hello)
        pl.semaphore_wait(barrier, self.n - 1)

    def put(self, lane, source, target, device):
        pltpu.make_async_remote_copy(
            src_ref=source,
            dst_ref=target,
            send_sem=self.send.at[lane],
            recv_sem=self.recv.at[lane],
            device_id=self.where(device),
            device_id_type=MESH,
        ).start()

    def keep(self, lane, source, target):
        pltpu.make_async_copy(source, target, self.local.at[lane]).start()

    def give(self, lane, source, target, device):
        @pl.when(device != self.me)
        def _():
            self.put(lane, source, target, device)

        @pl.when(device == self.me)
        def _():
            self.keep(lane, source, target)

    def kept(self, lane, like):
        pltpu.make_async_copy(like, like, self.local.at[lane]).wait()

    def sent(self, lane, like):
        pltpu.make_async_copy(like, like, self.send.at[lane]).wait()

    def came(self, lane, like):
        pltpu.make_async_copy(like, like, self.recv.at[lane]).wait()

    def settle(self, lane, like):
        self.came(lane, like)
        self.sent(lane, like)

    def settle_given(self, lane, mine, less, whole):
        @pl.when(mine)
        def _():
            self.kept(lane, whole[0])
            self.settle(lane, less)

        @pl.when(jnp.logical_not(mine))
        def _():
            self.settle(lane, whole[1])

    def group(self, step):
        m = lax.rem(self.m + step, G)
        return m, self.t * G + m

    def column(self, step):
        t = lax.rem(self.t + step, self.sizes.groups)
        return t, t * G + self.m


class Gather:
    LANES = 4

    def __init__(self, wire, lane, block, place, four):
        self.wire, self.lane, self.block, self.place, self.four = wire, lane, block, place, four

    def start(self):
        wire, mine = self.wire, self.place(self.wire.m)
        for k, m in enumerate(wire.peers):
            wire.put(self.lane + k, self.block, mine, wire.t * G + m)
        wire.put(self.lane + 3, self.block, mine, wire.sibling)
        wire.keep(self.lane, self.block, mine)

    def forward(self):
        wire = self.wire
        for k, m in enumerate(wire.peers):
            wire.came(self.lane + k, self.place(m))
            wire.put(self.lane + 3, self.place(m), self.place(m), wire.sibling)

    def finish(self):
        wire = self.wire
        wire.kept(self.lane, self.place(wire.m))
        for k in range(3):
            wire.sent(self.lane + k, self.place(wire.m))
        wire.settle(self.lane + 3, self.four)


class Scatter:
    LANES = 4

    def __init__(self, wire, lane, parts, got, summed, result):
        self.wire, self.lane = wire, lane
        self.parts, self.got, self.summed, self.result = parts, got, summed, result

    def start(self):
        wire = self.wire
        for k, m in enumerate([wire.m] + wire.peers):
            wire.put(self.lane + 3, self.parts.at[flip(m, 2)], self.got.at[k], wire.sibling)

    def forward(self):
        wire = self.wire
        wire.came(self.lane + 3, self.got)
        rows = self.got.shape[1]
        step = 16
        for k, m in reversed(list(enumerate([wire.m] + wire.peers))):

            def add(i, k=k, m=m):
                at = span(i, step)
                total = self.parts[m, at, :].astype(F32) + self.got[k, at, :].astype(F32)
                self.summed[k, at, :] = total.astype(BF16)

            loop(0, rows // step, add)
            if k:
                wire.put(self.lane + k - 1, self.summed.at[k], self.result.at[k], wire.t * G + m)
            else:
                wire.keep(self.lane, self.summed.at[0], self.result.at[0])

    def finish(self):
        wire = self.wire
        wire.sent(self.lane + 3, self.got)
        wire.kept(self.lane, self.result.at[0])
        for k in range(3):
            wire.settle(self.lane + k, self.result.at[k + 1])


def scatter_scratch(rows, width):
    return [pltpu.VMEM((4, rows, width), BF16), pltpu.VMEM((4, rows, width), BF16)]


def exchange(body, name, number, sizes, lanes, inputs, outs, scratch=(), vmem_outs=0):
    def kernel(*refs):
        ins = refs[: len(inputs)]
        results = refs[len(inputs) : len(inputs) + len(outs)]
        extra = refs[len(inputs) + len(outs) : len(refs) - 3]
        wire = Wire(sizes, *refs[len(refs) - 3 :])
        wire.greet()
        body(wire, *ins, *results, *extra)

    kernel.__name__ = name
    return pl.pallas_call(
        kernel,
        out_shape=[jax.ShapeDtypeStruct(shape, kind) for shape, kind in outs],
        in_specs=[VMEM] * len(inputs),
        out_specs=[VMEM] * vmem_outs + [ANY] * (len(outs) - vmem_outs),
        scratch_shapes=[*scratch, *([pltpu.SemaphoreType.DMA((lanes,))] * 3)],
        compiler_params=pltpu.CompilerParams(collective_id=number, has_side_effects=True),
        name=name,
    )(*inputs)


def normalize(inputs):
    centred = inputs - jnp.mean(inputs, axis=1, keepdims=True)
    inverse = lax.rsqrt(jnp.mean(centred * centred, axis=1, keepdims=True) + EPSILON)
    return centred * inverse, inverse


def normalize_back(grad_norm, scaled, inverse, gain_row):
    grad_scaled = grad_norm * gain_row
    mean_one = jnp.mean(grad_scaled, axis=1, keepdims=True)
    mean_two = jnp.mean(grad_scaled * scaled, axis=1, keepdims=True)
    return inverse * (grad_scaled - mean_one - scaled * mean_two)


def gelu_pair(pre_act):
    tangent = jnp.tanh(GELU_SCALE * (pre_act + GELU_CUBIC * pre_act * pre_act * pre_act))
    activated = 0.5 * pre_act * (1.0 + tangent)
    derivative = 0.5 * (1.0 + tangent) + 0.5 * pre_act * (1.0 - tangent * tangent) * GELU_SCALE * (
        1.0 + 3.0 * GELU_CUBIC * pre_act * pre_act
    )
    return (activated, derivative)


def tiles_of(queries, parts):
    wide = min(256, queries)
    deep = min(512, wide * parts)
    return wide, deep, wide * parts // deep


def query_places(tile, wide, parts, part):
    column = lax.broadcasted_iota(jnp.int32, (1, wide), 1)
    block = tile * (wide // 128) + column // 128
    return (block * parts + part) * 128 + lax.rem(column, 128)


def attend_tiles(wire, query_ref, pair_ref, out_ref, total_ref, key_ref, after):
    width, queries = query_ref.shape
    keys = pair_ref.shape[2]
    parts = wire.sizes.parts
    wide, deep, band = tiles_of(queries, parts)
    factor = LOG2E / math.sqrt(width)

    def turn(j):
        at = span(j, deep)
        key_ref[at, :] = pair_ref[0, :, at].T

    loop(0, keys // deep, turn)

    def tile_step(tile):
        mine = span(tile, wide)
        query = query_ref[:, mine]
        places = query_places(tile, wide, parts, wire.part)

        def step(j, carry, masked):
            best, total, summed = carry
            at = span(j, deep)
            scores = dot(key_ref[at, :], query, 1, 0)
            if masked:
                key_places = j * deep + lax.broadcasted_iota(jnp.int32, (deep, wide), 0)
                scores = jnp.where(key_places <= places, scores, -1e30)
            higher = jnp.maximum(best, jnp.max(scores, axis=0, keepdims=True))
            weights = jnp.exp2((scores - higher) * factor)
            shrunk = jnp.exp2((best - higher) * factor)
            total = total * shrunk + jnp.sum(weights, axis=0, keepdims=True)
            summed = summed * shrunk + dot(pair_ref[1, :, at], weights.astype(BF16), 1, 0)
            return higher, total, summed

        carry = (
            jnp.full((1, wide), -1e30, F32),
            jnp.zeros((1, wide), F32),
            jnp.zeros((width, wide), F32),
        )
        carry = lax.fori_loop(0, tile * band, lambda j, c: step(j, c, False), carry)
        for extra in range(band):
            carry = step(tile * band + extra, carry, True)
        best, total, summed = carry
        out_ref[:, mine] = (summed / total).astype(BF16)
        total_ref[:, mine] = best * factor + jnp.log2(total)
        after(tile)

    loop(0, queries // wide, tile_step)


def attend_back_tiles(
    wire, query_ref, pair_ref, grad_ref, out_ref, total_ref, dq_ref, dpair_ref, query_rows, grad_rows, delta_ref, dq_sum, after
):
    width, queries = query_ref.shape
    keys = pair_ref.shape[2]
    parts = wire.sizes.parts
    wide, deep, band = tiles_of(queries, parts)
    scale = 1.0 / math.sqrt(width)
    factor = LOG2E * scale

    def prepare(tile):
        mine = span(tile, wide)
        grad = grad_ref[:, mine]
        query_rows[mine, :] = query_ref[:, mine].T
        grad_rows[mine, :] = grad.T
        delta_ref[:, mine] = jnp.sum(grad.astype(F32) * out_ref[:, mine].astype(F32), axis=0, keepdims=True)
        dq_sum[:, mine] = jnp.zeros((width, wide), F32)

    loop(0, queries // wide, prepare)

    def key_step(j):
        at = span(j, deep)
        key_t, value_t = pair_ref[0, :, at], pair_ref[1, :, at]
        key, value = key_t.T, value_t.T
        key_places = j * deep + lax.broadcasted_iota(jnp.int32, (deep, wide), 0)

        def step(tile, carry, masked):
            dkey, dvalue = carry
            mine = span(tile, wide)
            scores = dot(key, query_ref[:, mine], 1, 0) * factor
            if masked:
                places = query_places(tile, wide, parts, wire.part)
                scores = jnp.where(key_places <= places, scores, -1e30)
            probs = jnp.exp2(scores - total_ref[:, mine])
            dvalue = dvalue + dot(probs.astype(BF16), grad_rows[mine, :], 1, 0)
            grad_probs = dot(value, grad_ref[:, mine], 1, 0)
            grad_scores = (probs * (grad_probs - delta_ref[:, mine]) * scale).astype(BF16)
            dkey = dkey + dot(grad_scores, query_rows[mine, :], 1, 0)
            dq_sum[:, mine] += dot(key_t, grad_scores, 1, 0)
            return dkey, dvalue

        first = j // band
        carry = (jnp.zeros((deep, width), F32), jnp.zeros((deep, width), F32))
        carry = step(first, carry, True)
        dkey, dvalue = lax.fori_loop(first + 1, queries // wide, lambda i, c: step(i, c, False), carry)
        dpair_ref[0, :, at] = dkey.T
        dpair_ref[1, :, at] = dvalue.T

        @pl.when(lax.rem(j, band) == band - 1)
        def _():
            mine = span(first, wide)
            dq_ref[:, mine] = dq_sum[:, mine].astype(BF16)

        after(j, first, lax.rem(j, band) == band - 1)

    loop(0, keys // deep, key_step)


def layer(n, fsdp):
    sizes = Sizes(n, fsdp)
    groups, parts, per_group = sizes.groups, sizes.parts, sizes.per_group

    def on_device(
        residual_in,
        first_gain,
        first_shift,
        attend_weight,
        attend_bias,
        merge_weight,
        merge_bias,
        second_gain,
        second_shift,
        expand_weight,
        expand_bias,
        shrink_weight,
        shrink_bias,
        cotangent,
    ):
        rows, width = residual_in.shape
        depth = width // n
        hidden_rows = shrink_weight.shape[0]
        hidden_units = expand_weight.shape[1]
        slice_width = width // G
        slice_units = hidden_units // G
        blocks = slice_units // UNITS
        shares = UNITS // hidden_rows
        head = width // H
        group_rows = rows * G
        half = group_rows // 2
        tokens = rows * n
        queries = tokens // parts
        chunk = per_group * rows
        me = position(fsdp)
        member = lax.rem(me, G)

        small = (first_gain, first_shift, attend_bias, merge_bias, second_gain, second_shift, expand_bias, shrink_bias)
        counts = [s.shape[0] for s in small]
        packed_rows = -(-sum(counts) // 2048) * 16
        packed = jnp.pad(jnp.concatenate(small), (0, packed_rows * 128 - sum(counts))).reshape(packed_rows, 128)

        def unit_block(q, m):
            return span(q * G + m, UNITS)

        def gather_first(wire, x, attend, merge, vec, expand, x_all, attend_all, merge_all, vec_all, expand_all):
            me, t, m = wire.me, wire.t, wire.m
            x_gather = Gather(wire, 4, x, lambda k: x_all.at[k], x_all.at[pl.ds(0, 4)])
            x_gather.start()

            def attend_to(other, move):
                for p in range(3):
                    columns = pl.ds(pl.multiple_of(p * width + other * slice_width, 128), slice_width)
                    move(0, attend.at[:, columns], attend_all.at[me, :, pl.ds(p * slice_width, slice_width)])

            def to_all(step):
                device = lax.rem(me + step, n)
                attend_to(lax.rem(device, G), lambda lane, s, d: wire.put(lane, s, d, device))
                wire.put(1, vec, vec_all.at[me], device)

            def expand_to(other, move):
                for q in range(blocks):
                    move(3, expand.at[:, unit_block(q, other)], expand_all.at[m, :, pl.ds(q * UNITS, UNITS)])

            def to_group(step):
                other, device = wire.group(step)
                expand_to(other, lambda lane, s, d: wire.put(lane, s, d, device))

            def to_column(step):
                _, device = wire.column(step)
                wire.put(2, merge, merge_all.at[t], device)

            loop(1, n, to_all)
            loop(1, groups, to_column)
            loop(1, G, to_group)
            attend_to(m, wire.keep)
            wire.keep(1, vec, vec_all.at[me])
            wire.keep(2, merge, merge_all.at[t])
            expand_to(m, wire.keep)
            wire.kept(0, attend_all.at[0])
            wire.kept(1, vec_all.at[0])
            wire.kept(2, merge_all.at[0])
            wire.kept(3, expand_all.at[0])
            x_gather.forward()
            wire.settle(0, attend_all.at[pl.ds(0, n - 1)])
            wire.settle(1, vec_all.at[pl.ds(0, n - 1)])
            wire.settle(2, merge_all.at[pl.ds(0, groups - 1)])
            wire.settle(3, expand_all.at[pl.ds(0, G - 1)])
            x_gather.finish()

        x_all, attend_all, merge_all, vec_all, expand_group = exchange(
            gather_first,
            "gather_first",
            0,
            sizes,
            8,
            (residual_in, attend_weight, merge_weight, packed, expand_weight),
            (
                ((G, rows, width), BF16),
                ((n, depth, 3 * slice_width), BF16),
                ((groups, depth, width), BF16),
                ((n, packed_rows, 128), BF16),
                ((G, depth, slice_units), BF16),
            ),
        )
        flat = vec_all.reshape(n, packed_rows * 128)
        spots = [sum(counts[:k]) for k in range(len(counts))]
        gain_one, shift_one, attend_shift, merge_shift, gain_two, shift_two, expand_shift, shrink_shift = (
            flat[:, spot : spot + count].reshape(-1).astype(F32) for spot, count in zip(spots, counts)
        )
        attend_slice = attend_all.reshape(width, 3 * slice_width)

        scaled_group, _ = normalize(x_all.reshape(group_rows, width).astype(F32))
        input_one = (scaled_group * gain_one + shift_one).astype(BF16)
        bias_mine = jnp.concatenate(
            [
                lax.dynamic_slice_in_dim(attend_shift, member * slice_width, slice_width),
                jnp.zeros((slice_width,), F32),
                lax.dynamic_slice_in_dim(attend_shift, width + member * slice_width, slice_width),
            ]
        )
        projected = (dot(attend_slice, input_one, 0, 1) + bias_mine[:, None]).astype(BF16)
        projected = projected.reshape(3, 2, head, group_rows)

        def spread_heads(wire, qkv, merge, pair, query, merge_full):
            t, m, core = wire.t, wire.m, wire.core
            chips = sizes.chips
            own = core == wire.source_core
            merge_gather = Gather(wire, 3, merge, lambda k: merge_full.at[:, k], merge_full.at[:, pl.ds(0, 4)])
            first = 7

            def to_chip(step):
                other = lax.rem(core * 2 * chips + lax.rem(t + step, 2 * chips), groups)
                which = lax.rem(other // chips, 2)
                for c in range(2):
                    device = other * G + m + 2 * (c - core)
                    mine = pl.ds(pl.multiple_of(t * group_rows + c * half, 128), half)
                    for kind in range(2):
                        wire.give(first + t, qkv.at[1 + kind, which, :, pl.ds(c * half, half)], pair.at[kind, :, mine], device)

            def queries_to(step):
                other = lax.rem(core * 2 * chips + lax.rem(t + step, 2 * chips), groups)
                which = lax.rem(other // chips, 2)
                for c in range(2):
                    device = other * G + m + 2 * (c - core)
                    part = lax.rem(other, chips) * 2 + c
                    for i in range(per_group):
                        source = span(part + i * parts, rows)
                        target = span(t * per_group + i, rows)
                        wire.give(0, qkv.at[0, which, :, source], query.at[:, target], device)

            loop(0, 2 * chips, to_chip)
            loop(0, 2 * chips, queries_to)
            merge_gather.start()

            def pass_on(step):
                other = lax.rem(t + step, groups)
                piece = pair.at[:, :, pl.ds(pl.multiple_of(other * group_rows + core * half, 128), half)]
                here = jnp.logical_and(own, other == t)

                @pl.when(here)
                def _():
                    wire.kept(first + other, piece)

                @pl.when(jnp.logical_not(here))
                def _():
                    wire.came(first + other, piece)

                wire.put(1, piece, piece, wire.sibling)

            loop(0, groups, pass_on)
            merge_gather.forward()
            all_halves = pair.at[:, :, pl.ds(0, tokens // 2)]
            wire.settle(1, all_halves)
            merge_gather.finish()

            @pl.when(own)
            def _():
                wire.sent(first + t, pair.at[:, :, pl.ds(0, (groups - 1) * half)])
                wire.kept(0, query.at[:, pl.ds(0, chunk)])
                wire.settle(0, query.at[:, pl.ds(0, queries - chunk)])

            @pl.when(jnp.logical_not(own))
            def _():
                wire.sent(first + t, all_halves)
                wire.settle(0, query)

        pair_t, query_t, merge_full = exchange(
            spread_heads,
            "spread_heads",
            1,
            sizes,
            7 + groups,
            (projected, merge_all),
            (((2, head, tokens), BF16), ((head, queries), BF16), ((groups, G, depth, width), BF16)),
        )
        merge_full = merge_full.reshape(width, width)

        def attend(wire, query, pair, expand, cot, out, total, attended, expand_all, cot_all, keys_scratch):
            me, t = wire.me, wire.t
            cot_gather = Gather(wire, 2, cot, lambda k: cot_all.at[k], cot_all.at[pl.ds(0, 4)])

            def to_column(step):
                _, device = wire.column(step)
                wire.put(1, expand, expand_all.at[t], device)

            loop(1, groups, to_column)
            cot_gather.start()
            wire.keep(1, expand, expand_all.at[t])
            place = span(wire.head, head)
            wide = tiles_of(queries, parts)[0]

            def after(tile):
                for b in range(wide // rows):
                    block = tile * (wide // rows) + b
                    wire.give(0, out.at[:, span(block, rows)], attended.at[place, :], block * parts + wire.part)

                @pl.when(tile == queries // wide - 2)
                def _():
                    cot_gather.forward()

            attend_tiles(wire, query, pair, out, total, keys_scratch, after)
            mine = lax.rem(me, parts) == wire.part

            @pl.when(mine)
            def _():
                wire.kept(0, attended.at[pl.ds(0, head), :])
                wire.came(0, attended.at[pl.ds(0, width - head), :])
                wire.sent(0, out.at[:, pl.ds(0, queries - rows)])

            @pl.when(jnp.logical_not(mine))
            def _():
                wire.came(0, attended)
                wire.sent(0, out)

            wire.kept(1, expand_all.at[0])
            wire.settle(1, expand_all.at[pl.ds(0, groups - 1)])
            cot_gather.finish()

        out_t, log_total, attended_t, expand_all, cot_all = exchange(
            attend,
            "attend",
            2,
            sizes,
            6,
            (query_t, pair_t, expand_group, cotangent),
            (
                ((head, queries), BF16),
                ((1, queries), F32),
                ((width, rows), BF16),
                ((groups, G, depth, slice_units), BF16),
                ((G, rows, width), BF16),
            ),
            scratch=[pltpu.VMEM((tokens, head), BF16)],
            vmem_outs=2,
        )

        lines = jnp.stack([merge_shift, gain_two, shift_two])
        shift_units = lax.dynamic_index_in_dim(expand_shift.reshape(blocks, G, UNITS), member, 1, False).reshape(1, -1)
        pair_rows = 2 * rows

        def feed(
            wire, att, merge, x, cot, cot_all, expand, shrink, lines, shift,
            hidden, grad_hidden, grad_input, grad_att, shrunk, grad_expand, sums, unit_sums, shrink_grads,
            normed, normed_all, shrink_all, act, slope, grad_pre, scaled, inverse, two_send, got, two_own, summed, two_all, shrink_part,
        ):
            me, t, m = wire.me, wire.t, wire.m
            block = me // shares
            user = lax.rem(block, G)
            here = lax.rem(m, 2)
            pair = m // 2
            pairs = [pair, flip(pair, 2)]
            theirs = [flip(p, 1) for p in pairs]

            def to_users(step):
                other = lax.rem(t + step, groups)
                slot = block // G * shares + lax.rem(me, shares)
                wire.give(0, shrink, shrink_all.at[span(slot, hidden_rows), :], other * G + user)

            loop(0, groups, to_users)
            step = min(32, rows)
            hidden[...] = dot(att[...].T, merge[...], 1, 0)

            def first_norm(i):
                at = span(i, step)
                value = x[at, :].astype(F32) + (hidden[at, :] + lines[0:1, :])
                centred = value - jnp.mean(value, axis=1, keepdims=True)
                inv = lax.rsqrt(jnp.mean(centred * centred, axis=1, keepdims=True) + EPSILON)
                hidden[at, :] = value
                scaled[at, :] = centred * inv
                inverse[at, :] = inv
                normed[at, :] = (centred * inv * lines[1:2, :] + lines[2:3, :]).astype(BF16)

            loop(0, rows // step, first_norm)
            place = lambda k: normed_all.at[span(k, rows), :]
            for k, other in enumerate(wire.peers):
                wire.put(1 + k, normed, place(m), t * G + other)
            wire.put(4, normed, place(m), wire.sibling)
            wire.keep(1, normed, place(m))

            def enter(p):
                at = span(p, pair_rows)
                pre_act = dot(normed_all[at, :], expand[...], 1, 0) + shift[...]
                activated, derivative = gelu_pair(pre_act)
                act[at, :] = activated.astype(BF16)
                slope[at, :] = derivative

            def passed(k):
                other = wire.peers[k]
                wire.came(1 + k, place(other))
                wire.put(4, place(other), place(other), wire.sibling)

            wire.kept(1, place(m))
            passed(0)
            enter(pairs[0])
            passed(1)
            passed(2)
            enter(pairs[1])
            wire.came(4, normed_all.at[pl.ds(0, 4 * rows), :])
            enter(theirs[0])
            enter(theirs[1])

            def shrink_gradient(q):
                columns = span(q, UNITS)
                shrink_part[columns, :] = dot(act[:, columns].T, cot_all[...], 1, 0).astype(BF16)
                for s in range(shares):
                    piece = shrink_part.at[pl.ds(pl.multiple_of(q * UNITS + s * hidden_rows, hidden_rows), hidden_rows), :]
                    wire.give(5, piece, shrink_grads.at[t], (q * G + m) * shares + s)

            loop(0, blocks, shrink_gradient)
            wire.settle_given(
                0, user == m, shrink_all.at[pl.ds(0, slice_units - hidden_rows), :], (shrink, shrink_all)
            )
            unit_sums[...] = jnp.zeros((1, slice_units), F32)

            def leave(p):
                at = span(p, pair_rows)
                grad = dot(cot_all[at, :], shrink_all[...], 1, 1) * slope[at, :]
                unit_sums[...] += jnp.sum(grad, axis=0, keepdims=True)
                grad_pre[at, :] = grad.astype(BF16)
                return dot(grad_pre[at, :], expand[...], 1, 1)

            for a in (1, 0):
                two_send[a] = leave(theirs[a]).astype(BF16)
                wire.put(6 + a, two_send.at[a], got.at[a], wire.sibling)
            two_own[...] = leave(pairs[1])
            wire.came(7, got.at[1])
            summed[1] = (two_own[...] + got[1].astype(F32)).astype(BF16)
            wire.put(8, summed.at[1, span(here, rows), :], two_all.at[0], t * G + wire.peers[1])
            wire.put(9, summed.at[1, span(1 - here, rows), :], two_all.at[1], t * G + wire.peers[2])
            two_own[...] = leave(pairs[0])
            wire.came(6, got.at[0])
            away = span(1 - here, rows)
            summed[0, away, :] = (two_own[away, :] + got[0, away, :].astype(F32)).astype(BF16)
            wire.put(10, summed.at[0, away, :], two_all.at[2], t * G + wire.peers[0])

            def expand_gradient(c):
                columns = span(c, 256)
                grad_expand[columns, :] = dot(normed_all[:, columns].T, grad_pre[...], 1, 0).astype(BF16)

            loop(0, width // 256, expand_gradient)

            def forward_out(p):
                at = span(p, pair_rows)
                shrunk[at, :] = dot(act[at, :], shrink_all[...], 1, 0).astype(BF16)

            loop(0, 4, forward_out)
            for k in range(3):
                wire.came(8 + k, two_all.at[k])
            sums[...] = jnp.zeros(sums.shape, F32)

            def second_norm(i):
                at = span(i, step)
                mine = pl.ds(pl.multiple_of(here * rows + i * step, step), step)
                grad_two = two_own[mine, :] + got[0, mine, :].astype(F32)
                for k in range(3):
                    grad_two = grad_two + two_all[k, at, :].astype(F32)
                top = cot[at, :].astype(F32)
                unit = scaled[at, :]
                grad_scaled = grad_two * lines[1:2, :]
                mean_one = jnp.mean(grad_scaled, axis=1, keepdims=True)
                mean_two = jnp.mean(grad_scaled * unit, axis=1, keepdims=True)
                result = top + inverse[at, :] * (grad_scaled - mean_one - unit * mean_two)
                grad_hidden[at, :] = result
                grad_input[at, :] = result.astype(BF16)
                sums[0:1, :] += jnp.sum(result, axis=0, keepdims=True)
                sums[1:2, :] += jnp.sum(grad_two * unit, axis=0, keepdims=True)
                sums[2:3, :] += jnp.sum(grad_two, axis=0, keepdims=True)
                sums[3:4, :] += jnp.sum(top, axis=0, keepdims=True)

            loop(0, rows // step, second_norm)
            grad_att[...] = dot(merge[...], grad_input[...], 1, 1).astype(BF16)
            for k in range(3):
                wire.sent(1 + k, normed)
                wire.sent(8 + k, two_all.at[k])
            wire.sent(4, normed_all.at[pl.ds(0, 4 * rows), :])
            wire.sent(6, got.at[0])
            wire.sent(7, got.at[1])
            wire.settle_given(
                5, lax.rem(me // shares, G) == m, shrink_grads.at[pl.ds(0, groups - 1)], (shrink_grads.at[0], shrink_grads)
            )

        (
            hidden, grad_hidden, grad_hidden_input, grad_attended_t, shrunk_part, grad_expand_part, second_sums, grad_expand_shift, shrink_parts,
        ) = exchange(
            feed,
            "feed",
            3,
            sizes,
            11,
            (
                attended_t,
                merge_full,
                residual_in,
                cotangent,
                cot_all.reshape(group_rows, width),
                expand_all.reshape(width, slice_units),
                shrink_weight,
                lines,
                shift_units,
            ),
            (
                ((rows, width), F32),
                ((rows, width), F32),
                ((rows, width), BF16),
                ((width, rows), BF16),
                ((group_rows, width), BF16),
                ((width, slice_units), BF16),
                ((4, width), F32),
                ((1, slice_units), F32),
                ((groups, hidden_rows, width), BF16),
            ),
            scratch=[
                pltpu.VMEM((rows, width), BF16),
                pltpu.VMEM((group_rows, width), BF16),
                pltpu.VMEM((slice_units, width), BF16),
                pltpu.VMEM((group_rows, slice_units), BF16),
                pltpu.VMEM((group_rows, slice_units), F32),
                pltpu.VMEM((group_rows, slice_units), BF16),
                pltpu.VMEM((rows, width), F32),
                pltpu.VMEM((rows, 1), F32),
                pltpu.VMEM((2, pair_rows, width), BF16),
                pltpu.VMEM((2, pair_rows, width), BF16),
                pltpu.VMEM((pair_rows, width), F32),
                pltpu.VMEM((2, pair_rows, width), BF16),
                pltpu.VMEM((3, rows, width), BF16),
                pltpu.VMEM((slice_units, width), BF16),
            ],
            vmem_outs=8,
        )
        block_in = residual_in.astype(F32)
        grad_shrink_weight = jnp.sum(shrink_parts.astype(F32), axis=0)
        grad_merge_shift, grad_gain_two, grad_shift_two, grad_shrink_shift = (second_sums[k] for k in range(4))

        wide, deep, band = tiles_of(queries, parts)
        pairs = tokens // deep // 2

        def attend_back(
            wire, query, pair, grad_own, out, total, shrunk, hidden_grad, att, expand,
            dq_all, dpair_all, shrunk_all, hidden_all, att_all, expand_all,
            grad, dq, dpair, dpair_out, query_rows, grad_rows, delta, dq_sum, pair_got, got, summed,
        ):
            me, t, m = wire.me, wire.t, wire.m
            shrunk_scatter = Scatter(wire, 5, shrunk, got, summed, shrunk_all)
            hidden_gather = Gather(wire, 9, hidden_grad, lambda k: hidden_all.at[k], hidden_all.at[pl.ds(0, 4)])
            first_pair = 13
            own_part = lax.rem(me, parts)
            own_place = span(me // parts, rows)

            def to_head(step):
                h = lax.rem(step + me, H)
                source_m = h // 2
                source_core = lax.rem(source_m // 2, 2)
                chip = (source_core * 2 + lax.rem(h, 2)) * sizes.chips + own_part // 2
                device = chip * G + source_m + 2 * (lax.rem(own_part, 2) - source_core)
                wire.give(4, grad_own.at[span(h, head), :], grad.at[:, own_place], device)

            loop(0, H, to_head)
            shrunk_scatter.start()
            hidden_gather.start()
            place = pl.ds(pl.multiple_of(m * rows, 128), rows)

            def to_group(step):
                other, device = wire.group(step)
                wire.put(2, att.at[span(other, slice_width), :], att_all.at[:, place], device)

            loop(1, G, to_group)
            wire.keep(2, att.at[span(m, slice_width), :], att_all.at[:, place])
            shrunk_scatter.forward()
            mine = wire.part == own_part

            @pl.when(mine)
            def _():
                wire.kept(4, grad_own.at[pl.ds(0, head), :])
                wire.came(4, grad.at[:, pl.ds(0, queries - rows)])
                wire.sent(4, grad_own.at[pl.ds(0, width - head), :])

            @pl.when(jnp.logical_not(mine))
            def _():
                wire.came(4, grad)
                wire.sent(4, grad_own)

            def to_column(step):
                other, device = wire.column(step)
                wire.put(3, expand.at[other], expand_all.at[t], device)

            loop(1, groups, to_column)
            wire.keep(3, expand.at[t], expand_all.at[t])
            chip = lax.rem(t, sizes.chips)

            def hand_over(j):
                at = span(j, deep)
                dpair_out[:, :, at] = dpair[:, :, at].astype(BF16)
                wire.put(first_pair + j // 2, dpair_out.at[:, :, at], pair_got.at[j // 2], wire.sibling)

            def add_up(j):
                at = span(j, deep)
                wire.came(first_pair + j // 2, pair_got.at[j // 2])
                dpair_out[:, :, at] = (dpair[:, :, at] + pair_got[j // 2].astype(F32)).astype(BF16)
                place_in_group = pl.ds(pl.multiple_of(lax.rem(j * deep, group_rows), deep), deep)
                device = j * deep // group_rows * G + wire.source_m
                wire.give(0, dpair_out.at[:, :, at], dpair_all.at[chip, wire.which, :, :, place_in_group], device)

            def after(j, first, final):
                @pl.when(lax.rem(j, 2) != wire.core)
                def _():
                    hand_over(j)

                @pl.when(jnp.logical_and(lax.rem(j + 1, 2) == wire.core, j > 0))
                def _():
                    add_up(j - 1)

                @pl.when(final)
                def _():
                    for b in range(wide // rows):
                        block = first * (wide // rows) + b
                        owner = block * parts + wire.part
                        wire.give(
                            1,
                            dq.at[:, span(block, rows)],
                            dq_all.at[wire.which, :, span(lax.rem(owner, G), rows)],
                            owner // G * G + wire.source_m,
                        )

                @pl.when(j == 2 * pairs - 2)
                def _():
                    hidden_gather.forward()

            attend_back_tiles(
                wire, query, pair, grad, out, total, dq, dpair, query_rows, grad_rows, delta, dq_sum, after
            )

            @pl.when(wire.core == 1)
            def _():
                add_up(2 * pairs - 1)

            own = wire.core == wire.source_core
            wire_half = dpair_out.at[:, :, pl.ds(0, tokens // 2)]

            @pl.when(own)
            def _():
                wire.kept(0, dpair_out.at[:, :, pl.ds(0, deep)])
                wire.kept(1, dq.at[:, pl.ds(0, chunk)])
                wire.settle(0, dpair_out.at[:, :, pl.ds(0, tokens // 2 - deep)])
                wire.settle(1, dq.at[:, pl.ds(0, queries - chunk)])

            @pl.when(jnp.logical_not(own))
            def _():
                wire.settle(0, wire_half)
                wire.settle(1, dq)

            loop(0, pairs, lambda k: wire.sent(first_pair + k, pair_got.at[0]))
            wire.kept(2, att_all.at[:, pl.ds(0, rows)])
            wire.settle(2, att_all.at[:, pl.ds(0, group_rows - rows)])
            wire.kept(3, expand_all.at[0])
            wire.settle(3, expand_all.at[pl.ds(0, groups - 1)])
            shrunk_scatter.finish()
            hidden_gather.finish()

        dq_all, dpair_all, shrunk_parts, grad_all, att_all, expand_parts = exchange(
            attend_back,
            "attend_back",
            6,
            sizes,
            13 + pairs,
            (
                query_t,
                pair_t,
                grad_attended_t,
                out_t,
                log_total,
                shrunk_part.reshape(G, rows, width),
                grad_hidden_input,
                attended_t,
                grad_expand_part.reshape(groups, G * depth, slice_units),
            ),
            (
                ((2, head, group_rows), BF16),
                ((sizes.chips, 2, 2, head, group_rows), BF16),
                ((4, rows, width), BF16),
                ((G, rows, width), BF16),
                ((slice_width, group_rows), BF16),
                ((groups, G * depth, slice_units), BF16),
            ),
            scratch=[
                pltpu.VMEM((head, queries), BF16),
                pltpu.VMEM((head, queries), BF16),
                pltpu.VMEM((2, head, tokens), F32),
                pltpu.VMEM((2, head, tokens), BF16),
                pltpu.VMEM((queries, head), BF16),
                pltpu.VMEM((queries, head), BF16),
                pltpu.VMEM((1, queries), F32),
                pltpu.VMEM((head, queries), F32),
                pltpu.VMEM((pairs, 2, head, deep), BF16),
                *scatter_scratch(rows, width),
            ],
        )
        residual_out = (hidden + jnp.sum(shrunk_parts.astype(F32), axis=0) + shrink_shift).astype(BF16)
        grad_expand_group = jnp.sum(expand_parts.astype(F32), axis=0).astype(BF16).reshape(G, depth, slice_units)
        grad_pair = jnp.sum(dpair_all.astype(F32), axis=0)
        grad_projected = jnp.concatenate(
            [
                dq_all.astype(F32).reshape(slice_width, group_rows),
                grad_pair[:, 0].reshape(slice_width, group_rows),
                grad_pair[:, 1].reshape(slice_width, group_rows),
            ],
            axis=0,
        )
        grad_shift_mine = jnp.sum(grad_projected, axis=1)
        grad_projected = grad_projected.astype(BF16)
        grad_attend_part = dot(input_one, grad_projected, 0, 1).astype(BF16)
        grad_one_part = dot(grad_projected, attend_slice, 0, 1)
        grad_gain_one = jnp.sum(grad_one_part * scaled_group, axis=0)
        grad_shift_one = jnp.sum(grad_one_part, axis=0)
        grad_merge_part = dot(att_all, grad_all.reshape(group_rows, width), 1, 0).astype(BF16)

        grad_attend_shift = jnp.zeros((2 * width,), F32)
        grad_attend_shift = lax.dynamic_update_slice_in_dim(
            grad_attend_shift, grad_shift_mine[:slice_width], member * slice_width, 0
        )
        grad_attend_shift = lax.dynamic_update_slice_in_dim(
            grad_attend_shift, grad_shift_mine[2 * slice_width :], width + member * slice_width, 0
        )
        grad_expand_all = lax.dynamic_update_slice_in_dim(
            jnp.zeros((blocks, G, UNITS), F32), grad_expand_shift.reshape(blocks, 1, UNITS), member, 1
        ).reshape(-1)
        grads = (
            grad_gain_one,
            grad_shift_one,
            grad_attend_shift,
            grad_merge_shift,
            grad_gain_two,
            grad_shift_two,
            grad_expand_all,
            grad_shrink_shift,
        )
        total_size = sum(counts)
        vec_rows = -(-total_size // 1024) * 8
        packed_grads = jnp.pad(
            jnp.concatenate([g.reshape(n, -1) for g in grads], axis=1), ((0, 0), (0, vec_rows * 128 - total_size))
        ).reshape(n, vec_rows, 128)

        def scatter_first(wire, one, attend, merge, vec, expand, one_all, attend_all, merge_all, vec_all, expand_all, got, summed):
            me, t, m = wire.me, wire.t, wire.m
            one_scatter = Scatter(wire, 4, one, got, summed, one_all)
            one_scatter.start()

            def attend_to(device, move):
                for p in range(3):
                    columns = pl.ds(pl.multiple_of(p * width + m * slice_width, 128), slice_width)
                    move(1, attend.at[device, :, pl.ds(p * slice_width, slice_width)], attend_all.at[t, :, columns])

            def to_all(step):
                device = lax.rem(me + step, n)
                attend_to(device, lambda lane, s, d: wire.put(lane, s, d, device))
                wire.put(3, vec.at[device], vec_all.at[me], device)

            def to_owners(slot):
                wire.give(2, merge.at[slot], merge_all.at[t], m * groups + slot)

            def expand_to(other, move):
                for q in range(blocks):
                    move(0, expand.at[other, :, pl.ds(q * UNITS, UNITS)], expand_all.at[:, unit_block(q, m)])

            def to_group(step):
                other, device = wire.group(step)
                expand_to(other, lambda lane, s, d: wire.put(lane, s, d, device))

            loop(1, n // 2, to_all)
            one_scatter.forward()
            loop(n // 2, n, to_all)
            loop(0, groups, to_owners)
            loop(1, G, to_group)
            attend_to(me, wire.keep)
            expand_to(m, wire.keep)
            wire.keep(3, vec.at[me], vec_all.at[me])
            wire.kept(0, expand.at[0])
            wire.kept(1, attend.at[0])
            wire.kept(3, vec_all.at[0])
            wire.settle(0, expand.at[pl.ds(0, G - 1)])
            wire.settle(1, attend.at[pl.ds(0, n - 1)])
            wire.settle(3, vec_all.at[pl.ds(0, n - 1)])
            wire.settle_given(2, me // groups == m, merge_all.at[pl.ds(0, groups - 1)], (merge_all.at[0], merge_all))
            one_scatter.finish()

        one_parts, attend_parts, merge_parts, vec_parts, expand_whole = exchange(
            scatter_first,
            "scatter_first",
            7,
            sizes,
            8,
            (
                grad_one_part.astype(BF16).reshape(G, rows, width),
                grad_attend_part.reshape(n, depth, 3 * slice_width),
                grad_merge_part.reshape(groups, depth, width),
                packed_grads,
                grad_expand_group,
            ),
            (
                ((4, rows, width), BF16),
                ((groups, depth, 3 * width), BF16),
                ((groups, depth, width), BF16),
                ((n, vec_rows, 128), F32),
                ((depth, hidden_units), BF16),
            ),
            scratch=scatter_scratch(rows, width),
        )
        grad_one = jnp.sum(one_parts.astype(F32), axis=0)
        scaled_one, inverse_one = normalize(block_in)
        input_grad = grad_hidden + normalize_back(grad_one, scaled_one, inverse_one, gain_one)
        grad_attend_weight = jnp.sum(attend_parts.astype(F32), axis=0)
        grad_merge_weight = jnp.sum(merge_parts.astype(F32), axis=0)
        vec_sums = jnp.sum(vec_parts, axis=0).reshape(-1)
        (g_gain_one, g_shift_one, g_attend_bias, g_merge_bias, g_gain_two, g_shift_two, g_expand_bias, g_shrink_bias) = (
            vec_sums[spot : spot + count] for spot, count in zip(spots, counts)
        )
        return (
            residual_out,
            input_grad,
            g_gain_one,
            g_shift_one,
            grad_attend_weight,
            g_attend_bias,
            grad_merge_weight,
            g_merge_bias,
            g_gain_two,
            g_shift_two,
            expand_whole.astype(F32),
            g_expand_bias,
            grad_shrink_weight,
            g_shrink_bias,
        )

    return on_device


def solution(mesh):
    rows, line = P(("ctx", "fsdp"), None), P(("ctx", "fsdp"))
    n, fsdp = mesh.shape["ctx"] * mesh.shape["fsdp"], mesh.shape["fsdp"]
    return jax.shard_map(
        layer(n, fsdp),
        mesh=mesh,
        in_specs=(rows, line, line, rows, line, rows, line, line, line, rows, line, rows, line, rows),
        out_specs=(rows, rows, line, line, rows, line, rows, line, line, line, rows, line, rows, line),
        check_vma=False,
    )
```

```python
import math

import jax
import jax.numpy as jnp
from jax import lax
from jax.experimental import pallas as pl
from jax.experimental.pallas import tpu as pltpu
from jax.sharding import PartitionSpec as P

H = 16
G = 8
UNITS = 128
EPSILON = 1e-05
GELU_SCALE = 0.7978845608028654
GELU_CUBIC = 0.044715
LOG2E = 1.4426950408889634
MESH = pl.DeviceIdType.MESH
BF16 = jnp.bfloat16
F32 = jnp.float32
VMEM = pl.BlockSpec(memory_space=pltpu.VMEM)
ANY = pl.BlockSpec(memory_space=pl.ANY)


def position(fsdp):
    return lax.axis_index("ctx") * fsdp + lax.axis_index("fsdp")


def flip(number, bit):
    return number + bit - 2 * bit * lax.rem(number // bit, 2)


def span(index, size):
    return pl.ds(pl.multiple_of(index * size, size), size)


def loop(low, high, step):
    def turn(index, carry):
        step(index)
        return carry

    lax.fori_loop(low, high, turn, 0)


def dot(left, right, left_dim, right_dim):
    return lax.dot_general(
        left, right, (((left_dim,), (right_dim,)), ((), ())), preferred_element_type=F32
    )


class Sizes:
    def __init__(self, n, fsdp):
        self.n, self.fsdp = n, fsdp
        self.groups = n // G
        self.parts = self.groups // 2
        self.chips = self.groups // 4
        self.per_group = G // self.parts


class Wire:
    def __init__(self, sizes, send, recv, local):
        self.sizes = sizes
        self.n, self.fsdp = sizes.n, sizes.fsdp
        self.send, self.recv, self.local = send, recv, local
        self.me = position(self.fsdp)
        self.t, self.m = self.me // G, lax.rem(self.me, G)
        self.core = lax.rem(self.m // 2, 2)
        self.sibling = flip(self.me, 2)
        self.peers = [flip(self.m, 1), flip(self.m, 4), flip(flip(self.m, 1), 4)]
        self.quarter = self.t // sizes.chips
        self.part = lax.rem(self.t, sizes.chips) * 2 + self.core
        self.source_core = self.quarter // 2
        self.source_m = self.m + 2 * (self.source_core - self.core)
        self.which = lax.rem(self.quarter, 2)
        self.head = 2 * self.source_m + self.which

    def where(self, device):
        return (device // self.fsdp, lax.rem(device, self.fsdp))

    def greet(self):
        barrier = pltpu.get_barrier_semaphore()

        def hello(step):
            other = lax.rem(self.me + step, self.n)
            pl.semaphore_signal(barrier, inc=1, device_id=self.where(other), device_id_type=MESH)

        loop(1, self.n, hello)
        pl.semaphore_wait(barrier, self.n - 1)

    def put(self, lane, source, target, device):
        pltpu.make_async_remote_copy(
            src_ref=source,
            dst_ref=target,
            send_sem=self.send.at[lane],
            recv_sem=self.recv.at[lane],
            device_id=self.where(device),
            device_id_type=MESH,
        ).start()

    def keep(self, lane, source, target):
        pltpu.make_async_copy(source, target, self.local.at[lane]).start()

    def give(self, lane, source, target, device):
        @pl.when(device != self.me)
        def _():
            self.put(lane, source, target, device)

        @pl.when(device == self.me)
        def _():
            self.keep(lane, source, target)

    def kept(self, lane, like):
        pltpu.make_async_copy(like, like, self.local.at[lane]).wait()

    def sent(self, lane, like):
        pltpu.make_async_copy(like, like, self.send.at[lane]).wait()

    def came(self, lane, like):
        pltpu.make_async_copy(like, like, self.recv.at[lane]).wait()

    def settle(self, lane, like):
        self.came(lane, like)
        self.sent(lane, like)

    def settle_given(self, lane, mine, less, whole):
        @pl.when(mine)
        def _():
            self.kept(lane, whole[0])
            self.settle(lane, less)

        @pl.when(jnp.logical_not(mine))
        def _():
            self.settle(lane, whole[1])

    def group(self, step):
        m = lax.rem(self.m + step, G)
        return m, self.t * G + m

    def column(self, step):
        t = lax.rem(self.t + step, self.sizes.groups)
        return t, t * G + self.m


class Gather:
    LANES = 4

    def __init__(self, wire, lane, block, place, four):
        self.wire, self.lane, self.block, self.place, self.four = wire, lane, block, place, four

    def start(self):
        wire, mine = self.wire, self.place(self.wire.m)
        for k, m in enumerate(wire.peers):
            wire.put(self.lane + k, self.block, mine, wire.t * G + m)
        wire.put(self.lane + 3, self.block, mine, wire.sibling)
        wire.keep(self.lane, self.block, mine)

    def forward(self):
        wire = self.wire
        for k, m in enumerate(wire.peers):
            wire.came(self.lane + k, self.place(m))
            wire.put(self.lane + 3, self.place(m), self.place(m), wire.sibling)

    def finish(self):
        wire = self.wire
        wire.kept(self.lane, self.place(wire.m))
        for k in range(3):
            wire.sent(self.lane + k, self.place(wire.m))
        wire.settle(self.lane + 3, self.four)


class Relay:
    def __init__(self, wire, lane, shard, place):
        self.wire, self.lane, self.shard, self.place = wire, lane, shard, place
        self.groups = wire.sizes.groups
        self.upper = lax.rem(wire.t, 2)
        self.mate = flip(wire.t, 1)

    def start(self):
        wire, t = self.wire, self.wire.t
        mine = self.place(t)
        wire.put(self.lane + t, self.shard, mine, self.mate * G + wire.m)

        def to_pair(step):
            pair = lax.rem(t // 2 + step, self.groups // 2)
            near = 2 * pair + jnp.where(pair < t // 2, 1, 0)
            wire.put(self.lane + t, self.shard, mine, near * G + wire.m)

        loop(1, self.groups // 2, to_pair)
        wire.keep(self.lane, self.shard, mine)

    def passes(self, distance):
        source = self.wire.t + jnp.where(self.upper == 1, distance, -distance)
        return source, jnp.logical_and(source >= 0, source < self.groups)

    def forward(self, low, high):
        def one(distance):
            source, there = self.passes(distance)

            @pl.when(there)
            def _():
                here = self.place(source)
                self.wire.came(self.lane + source, here)
                self.wire.put(self.lane + source, here, here, self.mate * G + self.wire.m)

        loop(low, high, one)

    def arrive(self):
        wire, t = self.wire, self.wire.t
        wire.kept(self.lane, self.place(t))

        def one(step):
            source = lax.rem(t + step, self.groups)
            passed = jnp.where(self.upper == 1, source > t, source < t)

            @pl.when(jnp.logical_not(passed))
            def _():
                wire.came(self.lane + source, self.place(source))

        loop(1, self.groups, one)

    def finish(self, half):
        self.wire.sent(self.lane + self.wire.t, half)

        def one(distance):
            source, there = self.passes(distance)

            @pl.when(there)
            def _():
                self.wire.sent(self.lane + source, self.place(source))

        loop(1, self.groups, one)


class Collect:
    def __init__(self, wire, lane, parts, got, summed, result):
        self.wire, self.lane = wire, lane
        self.parts, self.got, self.summed, self.result = parts, got, summed, result
        self.groups = wire.sizes.groups
        self.upper = lax.rem(wire.t, 2)
        self.mate = flip(wire.t, 1)
        self.pair = wire.t // 2
        self.out = lane + self.groups + self.pair

    def passes(self, distance):
        target = self.wire.t + jnp.where(self.upper == 1, distance, -distance)
        return target, jnp.logical_and(target >= 0, target < self.groups)

    def leaves(self, distance):
        target = self.mate + jnp.where(self.upper == 1, -distance, distance)
        return target, jnp.logical_and(target >= 0, target < self.groups)

    def start(self, make=lambda target: None):
        wire = self.wire

        def one(distance):
            target, there = self.leaves(distance)

            @pl.when(there)
            def _():
                make(target)
                wire.put(self.lane + target, self.parts.at[target], self.got.at[target], self.mate * G + wire.m)

        loop(1, self.groups, one)
        make(self.mate)
        wire.put(self.out, self.parts.at[self.mate], self.result.at[self.pair], self.mate * G + wire.m)

        def other(distance):
            target, there = self.passes(distance)

            @pl.when(there)
            def _():
                make(target)

        loop(1, self.groups, other)
        make(wire.t)

    def forward(self, low, high):
        wire = self.wire
        rows = self.parts.shape[1]
        step = math.gcd(rows, 32)

        def one(distance):
            target, there = self.passes(distance)

            @pl.when(there)
            def _():
                wire.came(self.lane + target, self.got.at[target])

                def add(i):
                    at = span(i, step)
                    total = self.parts[target, at, :].astype(F32) + self.got[target, at, :].astype(F32)
                    self.summed[target, at, :] = total.astype(BF16)

                loop(0, rows // step, add)
                wire.put(self.out, self.summed.at[target], self.result.at[self.pair], target * G + wire.m)

        loop(low, high, one)

    def finish(self):
        wire = self.wire
        loop(0, self.groups // 2, lambda q: wire.came(self.lane + self.groups + q, self.result.at[q]))
        wire.sent(self.out, self.result.at[0])

        def one(distance):
            target, there = self.passes(distance)

            @pl.when(there)
            def _():
                wire.sent(self.out, self.result.at[0])

            gone, was = self.leaves(distance)

            @pl.when(was)
            def _():
                wire.sent(self.lane + gone, self.result.at[0])

        loop(1, self.groups, one)


class Scatter:
    LANES = 4

    def __init__(self, wire, lane, parts, got, summed, result):
        self.wire, self.lane = wire, lane
        self.parts, self.got, self.summed, self.result = parts, got, summed, result

    def start(self):
        wire = self.wire
        for k, m in enumerate([wire.m] + wire.peers):
            wire.put(self.lane + 3, self.parts.at[flip(m, 2)], self.got.at[k], wire.sibling)

    def forward(self):
        wire = self.wire
        wire.came(self.lane + 3, self.got)
        rows = self.got.shape[1]
        step = 16
        for k, m in reversed(list(enumerate([wire.m] + wire.peers))):

            def add(i, k=k, m=m):
                at = span(i, step)
                total = self.parts[m, at, :].astype(F32) + self.got[k, at, :].astype(F32)
                self.summed[k, at, :] = total.astype(BF16)

            loop(0, rows // step, add)
            if k:
                wire.put(self.lane + k - 1, self.summed.at[k], self.result.at[k], wire.t * G + m)
            else:
                wire.keep(self.lane, self.summed.at[0], self.result.at[0])

    def finish(self):
        wire = self.wire
        wire.sent(self.lane + 3, self.got)
        wire.kept(self.lane, self.result.at[0])
        for k in range(3):
            wire.settle(self.lane + k, self.result.at[k + 1])


def scatter_scratch(rows, width):
    return [pltpu.VMEM((4, rows, width), BF16), pltpu.VMEM((4, rows, width), BF16)]


def exchange(body, name, number, sizes, lanes, inputs, outs, scratch=(), vmem_outs=0):
    def kernel(*refs):
        ins = refs[: len(inputs)]
        results = refs[len(inputs) : len(inputs) + len(outs)]
        extra = refs[len(inputs) + len(outs) : len(refs) - 3]
        wire = Wire(sizes, *refs[len(refs) - 3 :])
        wire.greet()
        body(wire, *ins, *results, *extra)

    kernel.__name__ = name
    return pl.pallas_call(
        kernel,
        out_shape=[jax.ShapeDtypeStruct(shape, kind) for shape, kind in outs],
        in_specs=[VMEM] * len(inputs),
        out_specs=[VMEM] * vmem_outs + [ANY] * (len(outs) - vmem_outs),
        scratch_shapes=[*scratch, *([pltpu.SemaphoreType.DMA((lanes,))] * 3)],
        compiler_params=pltpu.CompilerParams(collective_id=number, has_side_effects=True),
        name=name,
    )(*inputs)


def normalize(inputs):
    centred = inputs - jnp.mean(inputs, axis=1, keepdims=True)
    inverse = lax.rsqrt(jnp.mean(centred * centred, axis=1, keepdims=True) + EPSILON)
    return centred * inverse, inverse


def normalize_back(grad_norm, scaled, inverse, gain_row):
    grad_scaled = grad_norm * gain_row
    mean_one = jnp.mean(grad_scaled, axis=1, keepdims=True)
    mean_two = jnp.mean(grad_scaled * scaled, axis=1, keepdims=True)
    return inverse * (grad_scaled - mean_one - scaled * mean_two)


def gelu_pair(pre_act):
    tangent = jnp.tanh(GELU_SCALE * (pre_act + GELU_CUBIC * pre_act * pre_act * pre_act))
    activated = 0.5 * pre_act * (1.0 + tangent)
    derivative = 0.5 * (1.0 + tangent) + 0.5 * pre_act * (1.0 - tangent * tangent) * GELU_SCALE * (
        1.0 + 3.0 * GELU_CUBIC * pre_act * pre_act
    )
    return (activated, derivative)


def tiles_of(queries, parts):
    wide = min(256, queries)
    deep = min(512, wide * parts)
    return wide, deep, wide * parts // deep


def query_places(tile, wide, parts, part):
    column = lax.broadcasted_iota(jnp.int32, (1, wide), 1)
    block = tile * (wide // 128) + column // 128
    return (block * parts + part) * 128 + lax.rem(column, 128)


def attend_tiles(wire, query_ref, pair_ref, out_ref, total_ref, key_ref, after):
    width, queries = query_ref.shape
    keys = pair_ref.shape[2]
    parts = wire.sizes.parts
    wide, deep, band = tiles_of(queries, parts)
    factor = LOG2E / math.sqrt(width)

    def turn(j):
        at = span(j, deep)
        key_ref[at, :] = pair_ref[0, :, at].T

    loop(0, keys // deep, turn)

    def tile_step(tile):
        mine = span(tile, wide)
        query = query_ref[:, mine]
        places = query_places(tile, wide, parts, wire.part)

        def step(j, carry, masked):
            best, total, summed = carry
            at = span(j, deep)
            scores = dot(key_ref[at, :], query, 1, 0)
            if masked:
                key_places = j * deep + lax.broadcasted_iota(jnp.int32, (deep, wide), 0)
                scores = jnp.where(key_places <= places, scores, -1e30)
            higher = jnp.maximum(best, jnp.max(scores, axis=0, keepdims=True))
            weights = jnp.exp2((scores - higher) * factor)
            shrunk = jnp.exp2((best - higher) * factor)
            total = total * shrunk + jnp.sum(weights, axis=0, keepdims=True)
            summed = summed * shrunk + dot(pair_ref[1, :, at], weights.astype(BF16), 1, 0)
            return higher, total, summed

        carry = (
            jnp.full((1, wide), -1e30, F32),
            jnp.zeros((1, wide), F32),
            jnp.zeros((width, wide), F32),
        )
        carry = lax.fori_loop(0, tile * band, lambda j, c: step(j, c, False), carry)
        for extra in range(band):
            carry = step(tile * band + extra, carry, True)
        best, total, summed = carry
        out_ref[:, mine] = (summed / total).astype(BF16)
        total_ref[:, mine] = best * factor + jnp.log2(total)
        after(tile)

    loop(0, queries // wide, tile_step)


def attend_back_tiles(
    wire, query_ref, pair_ref, grad_ref, out_ref, total_ref, dq_ref, dpair_ref, query_rows, grad_rows, delta_ref, dq_sum, after
):
    width, queries = query_ref.shape
    keys = pair_ref.shape[2]
    parts = wire.sizes.parts
    wide, deep, band = tiles_of(queries, parts)
    scale = 1.0 / math.sqrt(width)
    factor = LOG2E * scale

    def prepare(tile):
        mine = span(tile, wide)
        grad = grad_ref[:, mine]
        query_rows[mine, :] = query_ref[:, mine].T
        grad_rows[mine, :] = grad.T
        delta_ref[:, mine] = jnp.sum(grad.astype(F32) * out_ref[:, mine].astype(F32), axis=0, keepdims=True)
        dq_sum[:, mine] = jnp.zeros((width, wide), F32)

    loop(0, queries // wide, prepare)

    def key_step(j):
        at = span(j, deep)
        key_t, value_t = pair_ref[0, :, at], pair_ref[1, :, at]
        key, value = key_t.T, value_t.T
        key_places = j * deep + lax.broadcasted_iota(jnp.int32, (deep, wide), 0)

        def step(tile, carry, masked):
            dkey, dvalue = carry
            mine = span(tile, wide)
            scores = dot(key, query_ref[:, mine], 1, 0) * factor
            if masked:
                places = query_places(tile, wide, parts, wire.part)
                scores = jnp.where(key_places <= places, scores, -1e30)
            probs = jnp.exp2(scores - total_ref[:, mine])
            dvalue = dvalue + dot(probs.astype(BF16), grad_rows[mine, :], 1, 0)
            grad_probs = dot(value, grad_ref[:, mine], 1, 0)
            grad_scores = (probs * (grad_probs - delta_ref[:, mine]) * scale).astype(BF16)
            dkey = dkey + dot(grad_scores, query_rows[mine, :], 1, 0)
            dq_sum[:, mine] += dot(key_t, grad_scores, 1, 0)
            return dkey, dvalue

        first = j // band
        carry = (jnp.zeros((deep, width), F32), jnp.zeros((deep, width), F32))
        carry = step(first, carry, True)
        dkey, dvalue = lax.fori_loop(first + 1, queries // wide, lambda i, c: step(i, c, False), carry)
        dpair_ref[0, :, at] = dkey.T
        dpair_ref[1, :, at] = dvalue.T

        @pl.when(lax.rem(j, band) == band - 1)
        def _():
            mine = span(first, wide)
            dq_ref[:, mine] = dq_sum[:, mine].astype(BF16)

        after(j, first, lax.rem(j, band) == band - 1)

    loop(0, keys // deep, key_step)


def layer(n, fsdp):
    sizes = Sizes(n, fsdp)
    groups, parts, per_group = sizes.groups, sizes.parts, sizes.per_group

    def on_device(
        residual_in,
        first_gain,
        first_shift,
        attend_weight,
        attend_bias,
        merge_weight,
        merge_bias,
        second_gain,
        second_shift,
        expand_weight,
        expand_bias,
        shrink_weight,
        shrink_bias,
        cotangent,
    ):
        rows, width = residual_in.shape
        depth = width // n
        hidden_rows = shrink_weight.shape[0]
        hidden_units = expand_weight.shape[1]
        slice_width = width // G
        slice_units = hidden_units // G
        blocks = slice_units // UNITS
        shares = UNITS // hidden_rows
        head = width // H
        group_rows = rows * G
        half = group_rows // 2
        tokens = rows * n
        queries = tokens // parts
        chunk = per_group * rows
        me = position(fsdp)
        member = lax.rem(me, G)

        small = (first_gain, first_shift, attend_bias, merge_bias, second_gain, second_shift, expand_bias, shrink_bias)
        counts = [s.shape[0] for s in small]
        packed_rows = -(-sum(counts) // 1024) * 8
        packed = jnp.zeros((packed_rows * 128,), F32)
        for k, vector in enumerate(small):
            low = sum(counts[:k])
            packed = packed + jnp.pad(vector.astype(F32), (low, packed_rows * 128 - low - counts[k]))
        packed = packed.astype(BF16).reshape(packed_rows, 128)

        def unit_block(q, m):
            return span(q * G + m, UNITS)

        def gather_first(
            wire, x, attend, merge, vec, expand, x_all, attend_all, merge_all, vec_all, expand_all, attend_group
        ):
            me, t, m = wire.me, wire.t, wire.m

            def attend_to(other, move):
                for p in range(3):
                    columns = pl.ds(pl.multiple_of(p * width + other * slice_width, 128), slice_width)
                    move(0, attend.at[:, columns], attend_group.at[m, :, pl.ds(p * slice_width, slice_width)])

            def expand_to(other, move):
                for q in range(blocks):
                    move(3, expand.at[:, unit_block(q, other)], expand_all.at[m, :, pl.ds(q * UNITS, UNITS)])

            def to_group(step):
                other, device = wire.group(step)
                attend_to(other, lambda lane, s, d: wire.put(lane, s, d, device))

            def to_all(step):
                device = lax.rem(me + step, n)
                wire.put(1, vec, vec_all.at[me], device)

            def more_to_group(step):
                other, device = wire.group(step)
                expand_to(other, lambda lane, s, d: wire.put(lane, s, d, device))

            loop(1, G, to_group)
            merge_relay = Relay(wire, 8, merge, lambda k: merge_all.at[k])
            merge_relay.start()
            x_gather = Gather(wire, 4, x, lambda k: x_all.at[k], x_all.at[pl.ds(0, 4)])
            x_gather.start()
            attend_to(m, wire.keep)
            loop(1, n, to_all)
            loop(1, G, more_to_group)
            wire.keep(1, vec, vec_all.at[me])
            expand_to(m, wire.keep)
            wire.kept(0, attend_group.at[0])
            wire.settle(0, attend_group.at[pl.ds(0, G - 1)])
            attend_relay = Relay(wire, 8 + groups, attend_group, lambda k: attend_all.at[k])
            attend_relay.start()
            merge_relay.forward(1, groups)
            wire.kept(1, vec_all.at[0])
            wire.kept(3, expand_all.at[0])
            attend_relay.forward(1, 2)
            x_gather.forward()
            attend_relay.forward(2, groups)
            wire.settle(1, vec_all.at[pl.ds(0, n - 1)])
            wire.settle(3, expand_all.at[pl.ds(0, G - 1)])
            x_gather.finish()
            merge_relay.arrive()
            attend_relay.arrive()
            merge_relay.finish(merge_all.at[pl.ds(0, groups // 2)])
            attend_relay.finish(attend_all.at[pl.ds(0, groups // 2)])

        x_all, attend_all, merge_all, vec_all, expand_group = exchange(
            gather_first,
            "gather_first",
            0,
            sizes,
            8 + 2 * groups,
            (residual_in, attend_weight, merge_weight, packed, expand_weight),
            (
                ((G, rows, width), BF16),
                ((groups, G, depth, 3 * slice_width), BF16),
                ((groups, depth, width), BF16),
                ((n, packed_rows, 128), BF16),
                ((G, depth, slice_units), BF16),
            ),
            scratch=[pltpu.VMEM((G, depth, 3 * slice_width), BF16)],
        )
        flat = vec_all.reshape(n, packed_rows * 128)
        spots = [sum(counts[:k]) for k in range(len(counts))]
        gain_one, shift_one, attend_shift, merge_shift, gain_two, shift_two, expand_shift, shrink_shift = (
            flat[:, spot : spot + count].reshape(-1).astype(F32) for spot, count in zip(spots, counts)
        )
        attend_slice = attend_all.reshape(width, 3 * slice_width)

        scaled_group, _ = normalize(x_all.reshape(group_rows, width).astype(F32))
        input_one = (scaled_group * gain_one + shift_one).astype(BF16)
        input_one, scaled_group = lax.optimization_barrier((input_one, scaled_group.astype(BF16)))
        bias_mine = jnp.concatenate(
            [
                lax.dynamic_slice_in_dim(attend_shift, member * slice_width, slice_width),
                jnp.zeros((slice_width,), F32),
                lax.dynamic_slice_in_dim(attend_shift, width + member * slice_width, slice_width),
            ]
        )
        projected = (dot(attend_slice, input_one, 0, 1) + bias_mine[:, None]).astype(BF16)
        projected = projected.reshape(3, 2, head, group_rows)

        def spread_heads(wire, qkv, merge, pair, query, merge_full):
            t, m, core = wire.t, wire.m, wire.core
            chips = sizes.chips
            own = core == wire.source_core
            merge_gather = Gather(wire, 3, merge, lambda k: merge_full.at[:, k], merge_full.at[:, pl.ds(0, 4)])
            first = 7

            def to_chip(step):
                other = lax.rem(core * 2 * chips + lax.rem(t + step, 2 * chips), groups)
                which = lax.rem(other // chips, 2)
                for c in range(2):
                    device = other * G + m + 2 * (c - core)
                    mine = pl.ds(pl.multiple_of(t * group_rows + c * half, 128), half)
                    for kind in range(2):
                        wire.give(first + t, qkv.at[1 + kind, which, :, pl.ds(c * half, half)], pair.at[kind, :, mine], device)

            def queries_to(step):
                other = lax.rem(core * 2 * chips + lax.rem(t + step, 2 * chips), groups)
                which = lax.rem(other // chips, 2)
                for c in range(2):
                    device = other * G + m + 2 * (c - core)
                    part = lax.rem(other, chips) * 2 + c
                    for i in range(per_group):
                        source = span(part + i * parts, rows)
                        target = span(t * per_group + i, rows)
                        wire.give(0, qkv.at[0, which, :, source], query.at[:, target], device)

            loop(0, 2 * chips, to_chip)
            loop(0, 2 * chips, queries_to)
            merge_gather.start()

            def pass_on(step):
                other = lax.rem(t + step, groups)
                piece = pair.at[:, :, pl.ds(pl.multiple_of(other * group_rows + core * half, 128), half)]
                here = jnp.logical_and(own, other == t)

                @pl.when(here)
                def _():
                    wire.kept(first + other, piece)

                @pl.when(jnp.logical_not(here))
                def _():
                    wire.came(first + other, piece)

                wire.put(1, piece, piece, wire.sibling)

            loop(0, groups, pass_on)
            merge_gather.forward()
            all_halves = pair.at[:, :, pl.ds(0, tokens // 2)]
            wire.settle(1, all_halves)
            merge_gather.finish()

            @pl.when(own)
            def _():
                wire.sent(first + t, pair.at[:, :, pl.ds(0, (groups - 1) * half)])
                wire.kept(0, query.at[:, pl.ds(0, chunk)])
                wire.settle(0, query.at[:, pl.ds(0, queries - chunk)])

            @pl.when(jnp.logical_not(own))
            def _():
                wire.sent(first + t, all_halves)
                wire.settle(0, query)

        pair_t, query_t, merge_full = exchange(
            spread_heads,
            "spread_heads",
            1,
            sizes,
            7 + groups,
            (projected, merge_all),
            (((2, head, tokens), BF16), ((head, queries), BF16), ((groups, G, depth, width), BF16)),
        )
        merge_full = merge_full.reshape(width, width)

        def attend(wire, query, pair, expand, cot, out, total, attended, expand_all, cot_all, keys_scratch):
            me, t = wire.me, wire.t
            cot_gather = Gather(wire, 2, cot, lambda k: cot_all.at[k], cot_all.at[pl.ds(0, 4)])

            relay = Relay(wire, 6, expand, lambda k: expand_all.at[k])
            relay.start()
            cot_gather.start()
            place = span(wire.head, head)
            wide = tiles_of(queries, parts)[0]

            def after(tile):
                for b in range(wide // rows):
                    block = tile * (wide // rows) + b
                    wire.give(0, out.at[:, span(block, rows)], attended.at[place, :], block * parts + wire.part)

                for k in (1, 2):

                    @pl.when(tile == queries // wide - 4 + k)
                    def _(k=k):
                        relay.forward(k, k + 1)

                @pl.when(tile == queries // wide - 2)
                def _():
                    cot_gather.forward()

            attend_tiles(wire, query, pair, out, total, keys_scratch, after)
            mine = lax.rem(me, parts) == wire.part

            @pl.when(mine)
            def _():
                wire.kept(0, attended.at[pl.ds(0, head), :])
                wire.came(0, attended.at[pl.ds(0, width - head), :])
                wire.sent(0, out.at[:, pl.ds(0, queries - rows)])

            @pl.when(jnp.logical_not(mine))
            def _():
                wire.came(0, attended)
                wire.sent(0, out)

            relay.forward(3, groups)
            relay.arrive()
            relay.finish(expand_all.at[pl.ds(0, groups // 2)])
            cot_gather.finish()

        out_t, log_total, attended_t, expand_all, cot_all = exchange(
            attend,
            "attend",
            2,
            sizes,
            6 + groups,
            (query_t, pair_t, expand_group, cotangent),
            (
                ((head, queries), BF16),
                ((1, queries), F32),
                ((width, rows), BF16),
                ((groups, G, depth, slice_units), BF16),
                ((G, rows, width), BF16),
            ),
            scratch=[pltpu.VMEM((tokens, head), BF16)],
            vmem_outs=2,
        )

        lines = jnp.stack([merge_shift, gain_two, shift_two])
        shift_units = lax.dynamic_index_in_dim(expand_shift.reshape(blocks, G, UNITS), member, 1, False).reshape(1, -1)
        pair_rows = 2 * rows

        def feed(
            wire, att, merge, x, cot, cot_all, expand, shrink, lines, shift,
            hidden, grad_hidden, grad_input, grad_att, shrunk, grad_expand, sums, unit_sums, shrink_own, shrink_grads,
            normed, normed_all, shrink_all, act, slope, grad_pre, scaled, inverse, two_send, got, two_own, summed, two_all, shrink_part,
            part_got, part_sum,
        ):
            me, t, m = wire.me, wire.t, wire.m
            block = me // shares
            user = lax.rem(block, G)
            here = lax.rem(m, 2)
            pair = m // 2
            pairs = [pair, flip(pair, 2)]
            theirs = [flip(p, 1) for p in pairs]

            def to_users(step):
                other = lax.rem(t + step, groups)
                slot = block // G * shares + lax.rem(me, shares)
                wire.give(0, shrink, shrink_all.at[span(slot, hidden_rows), :], other * G + user)

            if shares == 1:
                relay = Relay(wire, 11, shrink, lambda k: shrink_all.at[span(k, hidden_rows), :])
                collect = Collect(wire, 11 + groups, shrink_part, part_got, part_sum, shrink_grads)
                relay.start()
            else:
                loop(0, groups, to_users)
            step = min(32, rows)
            hidden[...] = dot(att[...].T, merge[...], 1, 0)

            def first_norm(i):
                at = span(i, step)
                value = x[at, :].astype(F32) + (hidden[at, :] + lines[0:1, :])
                centred = value - jnp.mean(value, axis=1, keepdims=True)
                inv = lax.rsqrt(jnp.mean(centred * centred, axis=1, keepdims=True) + EPSILON)
                hidden[at, :] = value
                scaled[at, :] = centred * inv
                inverse[at, :] = inv
                normed[at, :] = (centred * inv * lines[1:2, :] + lines[2:3, :]).astype(BF16)

            loop(0, rows // step, first_norm)
            place = lambda k: normed_all.at[span(k, rows), :]
            for k, other in enumerate(wire.peers):
                wire.put(1 + k, normed, place(m), t * G + other)
            wire.put(4, normed, place(m), wire.sibling)
            wire.keep(1, normed, place(m))

            def enter(p):
                at = span(p, pair_rows)
                pre_act = dot(normed_all[at, :], expand[...], 1, 0) + shift[...]
                activated, derivative = gelu_pair(pre_act)
                act[at, :] = activated.astype(BF16)
                slope[at, :] = derivative

            def passed(k):
                other = wire.peers[k]
                wire.came(1 + k, place(other))
                wire.put(4, place(other), place(other), wire.sibling)

            wire.kept(1, place(m))
            passed(0)
            if shares == 1:
                relay.forward(1, 2)
            enter(pairs[0])
            passed(1)
            passed(2)
            if shares == 1:
                relay.forward(2, groups)
            enter(pairs[1])
            wire.came(4, normed_all.at[pl.ds(0, 4 * rows), :])
            enter(theirs[0])
            enter(theirs[1])

            def shrink_gradient(q):
                columns = span(q, UNITS)
                total = dot(act[:, columns].T, cot_all[...], 1, 0)
                for s in range(shares):
                    piece = q * shares + s
                    shrink_part[piece] = total[s * hidden_rows : (s + 1) * hidden_rows, :].astype(BF16)
                    if shares > 1:
                        wire.give(5, shrink_part.at[piece], shrink_grads.at[t], (q * G + m) * shares + s)

            loop(0, blocks, shrink_gradient)
            if shares == 1:
                collect.start()
                relay.arrive()
            else:
                wire.settle_given(
                    0, user == m, shrink_all.at[pl.ds(0, slice_units - hidden_rows), :], (shrink, shrink_all)
                )
            unit_sums[...] = jnp.zeros((1, slice_units), F32)

            def leave(p):
                at = span(p, pair_rows)
                grad = dot(cot_all[at, :], shrink_all[...], 1, 1) * slope[at, :]
                unit_sums[...] += jnp.sum(grad, axis=0, keepdims=True)
                grad_pre[at, :] = grad.astype(BF16)
                return dot(grad_pre[at, :], expand[...], 1, 1)

            for a in (1, 0):
                two_send[a] = leave(theirs[a]).astype(BF16)
                wire.put(6 + a, two_send.at[a], got.at[a], wire.sibling)
            if shares == 1:
                collect.forward(1, 2)
            two_own[...] = leave(pairs[1])
            wire.came(7, got.at[1])
            summed[1] = (two_own[...] + got[1].astype(F32)).astype(BF16)
            wire.put(8, summed.at[1, span(here, rows), :], two_all.at[0], t * G + wire.peers[1])
            wire.put(9, summed.at[1, span(1 - here, rows), :], two_all.at[1], t * G + wire.peers[2])
            two_own[...] = leave(pairs[0])
            wire.came(6, got.at[0])
            away = span(1 - here, rows)
            summed[0, away, :] = (two_own[away, :] + got[0, away, :].astype(F32)).astype(BF16)
            wire.put(10, summed.at[0, away, :], two_all.at[2], t * G + wire.peers[0])

            if shares == 1:
                collect.forward(2, groups)

            def expand_gradient(c):
                columns = span(c, 256)
                grad_expand[columns, :] = dot(normed_all[:, columns].T, grad_pre[...], 1, 0).astype(BF16)

            loop(0, width // 256, expand_gradient)

            def forward_out(p):
                at = span(p, pair_rows)
                shrunk[at, :] = dot(act[at, :], shrink_all[...], 1, 0).astype(BF16)

            loop(0, 4, forward_out)
            for k in range(3):
                wire.came(8 + k, two_all.at[k])
            sums[...] = jnp.zeros(sums.shape, F32)

            def second_norm(i):
                at = span(i, step)
                mine = pl.ds(pl.multiple_of(here * rows + i * step, step), step)
                grad_two = two_own[mine, :] + got[0, mine, :].astype(F32)
                for k in range(3):
                    grad_two = grad_two + two_all[k, at, :].astype(F32)
                top = cot[at, :].astype(F32)
                unit = scaled[at, :]
                grad_scaled = grad_two * lines[1:2, :]
                mean_one = jnp.mean(grad_scaled, axis=1, keepdims=True)
                mean_two = jnp.mean(grad_scaled * unit, axis=1, keepdims=True)
                result = top + inverse[at, :] * (grad_scaled - mean_one - unit * mean_two)
                grad_hidden[at, :] = result
                grad_input[at, :] = result.astype(BF16)
                sums[0:1, :] += jnp.sum(result, axis=0, keepdims=True)
                sums[1:2, :] += jnp.sum(grad_two * unit, axis=0, keepdims=True)
                sums[2:3, :] += jnp.sum(grad_two, axis=0, keepdims=True)
                sums[3:4, :] += jnp.sum(top, axis=0, keepdims=True)

            loop(0, rows // step, second_norm)
            grad_att[...] = dot(merge[...], grad_input[...], 1, 1).astype(BF16)
            for k in range(3):
                wire.sent(1 + k, normed)
                wire.sent(8 + k, two_all.at[k])
            wire.sent(4, normed_all.at[pl.ds(0, 4 * rows), :])
            wire.sent(6, got.at[0])
            wire.sent(7, got.at[1])
            if shares == 1:
                relay.finish(shrink_all.at[pl.ds(0, groups // 2 * hidden_rows), :])
                collect.finish()
                shrink_own[...] = shrink_part[t]
            else:
                shrink_own[...] = jnp.zeros(shrink_own.shape, BF16)
                wire.settle_given(
                    5, lax.rem(me // shares, G) == m, shrink_grads.at[pl.ds(0, groups - 1)], (shrink_grads.at[0], shrink_grads)
                )

        shrink_terms = groups // 2 if shares == 1 else groups
        (
            hidden, grad_hidden, grad_hidden_input, grad_attended_t, shrunk_part, grad_expand_part, second_sums, grad_expand_shift, shrink_own, shrink_parts,
        ) = exchange(
            feed,
            "feed",
            3,
            sizes,
            11 + groups + groups * 3 // 2,
            (
                attended_t,
                merge_full,
                residual_in,
                cotangent,
                cot_all.reshape(group_rows, width),
                expand_all.reshape(width, slice_units),
                shrink_weight,
                lines,
                shift_units,
            ),
            (
                ((rows, width), F32),
                ((rows, width), F32),
                ((rows, width), BF16),
                ((width, rows), BF16),
                ((group_rows, width), BF16),
                ((width, slice_units), BF16),
                ((4, width), F32),
                ((1, slice_units), F32),
                ((hidden_rows, width), BF16),
                ((shrink_terms, hidden_rows, width), BF16),
            ),
            scratch=[
                pltpu.VMEM((rows, width), BF16),
                pltpu.VMEM((group_rows, width), BF16),
                pltpu.VMEM((slice_units, width), BF16),
                pltpu.VMEM((group_rows, slice_units), BF16),
                pltpu.VMEM((group_rows, slice_units), F32),
                pltpu.VMEM((group_rows, slice_units), BF16),
                pltpu.VMEM((rows, width), F32),
                pltpu.VMEM((rows, 1), F32),
                pltpu.VMEM((2, pair_rows, width), BF16),
                pltpu.VMEM((2, pair_rows, width), BF16),
                pltpu.VMEM((pair_rows, width), F32),
                pltpu.VMEM((2, pair_rows, width), BF16),
                pltpu.VMEM((3, rows, width), BF16),
                *([pltpu.VMEM((groups, hidden_rows, width), BF16)] * 3),
            ],
            vmem_outs=9,
        )
        wide, deep, band = tiles_of(queries, parts)
        pairs = tokens // deep // 2

        def attend_back(
            wire, query, pair, grad_own, out, total, shrunk, hidden_grad, att, expand,
            dq_all, dpair_all, shrunk_all, hidden_all, att_all, expand_all,
            grad, dq, dpair, dpair_out, query_rows, grad_rows, delta, dq_sum, pair_got, got, summed, part_got, part_sum,
        ):
            me, t, m = wire.me, wire.t, wire.m
            shrunk_scatter = Scatter(wire, 5, shrunk, got, summed, shrunk_all)
            hidden_gather = Gather(wire, 9, hidden_grad, lambda k: hidden_all.at[k], hidden_all.at[pl.ds(0, 4)])
            first_pair = 13
            own_part = lax.rem(me, parts)
            own_place = span(me // parts, rows)

            def to_head(step):
                h = lax.rem(step + me, H)
                source_m = h // 2
                source_core = lax.rem(source_m // 2, 2)
                chip = (source_core * 2 + lax.rem(h, 2)) * sizes.chips + own_part // 2
                device = chip * G + source_m + 2 * (lax.rem(own_part, 2) - source_core)
                wire.give(4, grad_own.at[span(h, head), :], grad.at[:, own_place], device)

            loop(0, H, to_head)
            shrunk_scatter.start()
            hidden_gather.start()
            place = pl.ds(pl.multiple_of(m * rows, 128), rows)

            def to_group(step):
                other, device = wire.group(step)
                wire.put(2, att.at[span(other, slice_width), :], att_all.at[:, place], device)

            loop(1, G, to_group)
            wire.keep(2, att.at[span(m, slice_width), :], att_all.at[:, place])
            shrunk_scatter.forward()
            mine = wire.part == own_part

            @pl.when(mine)
            def _():
                wire.kept(4, grad_own.at[pl.ds(0, head), :])
                wire.came(4, grad.at[:, pl.ds(0, queries - rows)])
                wire.sent(4, grad_own.at[pl.ds(0, width - head), :])

            @pl.when(jnp.logical_not(mine))
            def _():
                wire.came(4, grad)
                wire.sent(4, grad_own)

            collect = Collect(wire, 13 + pairs, expand, part_got, part_sum, expand_all)
            collect.start()
            chip = lax.rem(t, sizes.chips)

            def hand_over(j):
                at = span(j, deep)
                dpair_out[:, :, at] = dpair[:, :, at].astype(BF16)
                wire.put(first_pair + j // 2, dpair_out.at[:, :, at], pair_got.at[j // 2], wire.sibling)

            def add_up(j):
                at = span(j, deep)
                wire.came(first_pair + j // 2, pair_got.at[j // 2])
                dpair_out[:, :, at] = (dpair[:, :, at] + pair_got[j // 2].astype(F32)).astype(BF16)
                place_in_group = pl.ds(pl.multiple_of(lax.rem(j * deep, group_rows), deep), deep)
                device = j * deep // group_rows * G + wire.source_m
                wire.give(0, dpair_out.at[:, :, at], dpair_all.at[chip, wire.which, :, :, place_in_group], device)

            def after(j, first, final):
                @pl.when(lax.rem(j, 2) != wire.core)
                def _():
                    hand_over(j)

                @pl.when(jnp.logical_and(lax.rem(j + 1, 2) == wire.core, j > 0))
                def _():
                    add_up(j - 1)

                @pl.when(final)
                def _():
                    for b in range(wide // rows):
                        block = first * (wide // rows) + b
                        owner = block * parts + wire.part
                        wire.give(
                            1,
                            dq.at[:, span(block, rows)],
                            dq_all.at[wire.which, :, span(lax.rem(owner, G), rows)],
                            owner // G * G + wire.source_m,
                        )

                for k in (1, 2):

                    @pl.when(j == k)
                    def _(k=k):
                        collect.forward(k, k + 1)

                @pl.when(j == 2 * pairs - 2)
                def _():
                    hidden_gather.forward()

            attend_back_tiles(
                wire, query, pair, grad, out, total, dq, dpair, query_rows, grad_rows, delta, dq_sum, after
            )

            @pl.when(wire.core == 1)
            def _():
                add_up(2 * pairs - 1)

            own = wire.core == wire.source_core
            wire_half = dpair_out.at[:, :, pl.ds(0, tokens // 2)]

            @pl.when(own)
            def _():
                wire.kept(0, dpair_out.at[:, :, pl.ds(0, deep)])
                wire.kept(1, dq.at[:, pl.ds(0, chunk)])
                wire.settle(0, dpair_out.at[:, :, pl.ds(0, tokens // 2 - deep)])
                wire.settle(1, dq.at[:, pl.ds(0, queries - chunk)])

            @pl.when(jnp.logical_not(own))
            def _():
                wire.settle(0, wire_half)
                wire.settle(1, dq)

            loop(0, pairs, lambda k: wire.sent(first_pair + k, pair_got.at[0]))
            wire.kept(2, att_all.at[:, pl.ds(0, rows)])
            wire.settle(2, att_all.at[:, pl.ds(0, group_rows - rows)])
            collect.forward(3, groups)
            collect.finish()
            shrunk_scatter.finish()
            hidden_gather.finish()

        dq_all, dpair_all, shrunk_parts, grad_all, att_all, expand_parts = exchange(
            attend_back,
            "attend_back",
            6,
            sizes,
            13 + pairs + groups * 3 // 2,
            (
                query_t,
                pair_t,
                grad_attended_t,
                out_t,
                log_total,
                shrunk_part.reshape(G, rows, width),
                grad_hidden_input,
                attended_t,
                grad_expand_part.reshape(groups, G * depth, slice_units),
            ),
            (
                ((2, head, group_rows), BF16),
                ((sizes.chips, 2, 2, head, group_rows), BF16),
                ((4, rows, width), BF16),
                ((G, rows, width), BF16),
                ((slice_width, group_rows), BF16),
                ((groups // 2, G * depth, slice_units), BF16),
            ),
            scratch=[
                pltpu.VMEM((head, queries), BF16),
                pltpu.VMEM((head, queries), BF16),
                pltpu.VMEM((2, head, tokens), F32),
                pltpu.VMEM((2, head, tokens), BF16),
                pltpu.VMEM((queries, head), BF16),
                pltpu.VMEM((queries, head), BF16),
                pltpu.VMEM((1, queries), F32),
                pltpu.VMEM((head, queries), F32),
                pltpu.VMEM((pairs, 2, head, deep), BF16),
                *scatter_scratch(rows, width),
                *([pltpu.VMEM((groups, G * depth, slice_units), BF16)] * 2),
            ],
        )
        owners = slice_width // depth

        def close(
            wire, dq, dpair, entered, unit, attend, att, grad, expand, expand_own, second, unit_sums,
            one_own, one_all, attend_all, merge_all, main_all, bias_all, unit_all, expand_all,
            projected, projected_rows, attend_part, part_got, part_sum, part_all, attend_own, merge_part, expand_part,
            vec, vec_got, vec_sum, send, got, summed,
        ):
            me, t, m = wire.me, wire.t, wire.m
            projected[pl.ds(0, slice_width), :] = dq[...]
            for which in range(2):
                for kind in range(2):
                    total = dpair[0, which, kind].astype(F32)
                    for chip in range(1, sizes.chips):
                        total = total + dpair[chip, which, kind].astype(F32)
                    projected[pl.ds((1 + kind) * slice_width + which * head, head), :] = total.astype(BF16)
            for p in range(3):
                part = pl.ds(p * slice_width, slice_width)
                projected_rows[:, part] = projected[part, :].T

            def attend_gradient(target):
                size = G * depth
                if size % 128 == 0:
                    total = dot(entered[:, span(target, size)].T, projected_rows[...], 1, 0)
                else:
                    both = dot(entered[:, span(target // 2, 128)].T, projected_rows[...], 1, 0)
                    total = jnp.where(lax.rem(target, 2) == 0, both[:size], both[size:])
                attend_part[target] = total.astype(BF16)

            collect = Collect(wire, 12, attend_part, part_got, part_sum, part_all)
            collect.start(attend_gradient)
            here = lax.rem(m, 2)
            pairs = [m // 2, flip(m // 2, 2)]
            vec[...] = jnp.zeros(vec.shape, F32)

            def leave(p):
                at = span(p, pair_rows)
                result = dot(projected_rows[at, :], attend[...], 1, 1)
                vec[0:1, :] += jnp.sum(result * unit[at, :].astype(F32), axis=0, keepdims=True)
                vec[1:2, :] += jnp.sum(result, axis=0, keepdims=True)
                return result

            for a in (1, 0):
                send[a] = leave(flip(pairs[a], 1)).astype(BF16)
                wire.put(4 + a, send.at[a], got.at[a], wire.sibling)
            result = leave(pairs[1])
            wire.came(5, got.at[1])
            collect.forward(1, 2)
            summed[1] = (result + got[1].astype(F32)).astype(BF16)
            wire.put(6, summed.at[1, span(here, rows), :], one_all.at[0], t * G + wire.peers[1])
            wire.put(7, summed.at[1, span(1 - here, rows), :], one_all.at[1], t * G + wire.peers[2])
            result = leave(pairs[0])
            wire.came(4, got.at[0])
            result = result + got[0].astype(F32)
            summed[0] = result.astype(BF16)
            wire.put(8, summed.at[0, span(1 - here, rows), :], one_all.at[2], t * G + wire.peers[0])

            shift = dot(jnp.ones((8, group_rows), BF16), projected[...], 1, 1)
            mine = span(m, 128)
            vec[2:3, mine] = shift[0:1, :slice_width]
            vec[3:4, mine] = shift[0:1, 2 * slice_width :]
            vec[4:8, :] = second[...]
            for q in range(blocks):
                vec[8 + q : 9 + q, mine] = unit_sums[:, q * UNITS : (q + 1) * UNITS]

            def lanes_to(step):
                other, device = wire.group(step)
                wire.put(3, vec.at[:, span(other, 128)], vec_got.at[m], device)

            loop(1, G, lanes_to)
            wire.keep(3, vec.at[:, mine], vec_got.at[m])
            collect.forward(2, groups)

            merged = dot(att[...], grad[...], 1, 0)
            for slot in range(groups):
                merge_part[slot] = merged[slot * depth : (slot + 1) * depth, :].astype(BF16)
                wire.give(2, merge_part.at[slot], merge_all.at[t], m * groups + slot)
            for other in range(G):
                total = expand_own[t, pl.ds(other * depth, depth), :].astype(F32)
                for k in range(groups // 2):
                    total = total + expand[k, pl.ds(other * depth, depth), :].astype(F32)
                expand_part[other] = total.astype(BF16)
                for q in range(blocks):
                    wire.give(
                        0,
                        expand_part.at[other, :, pl.ds(q * UNITS, UNITS)],
                        expand_all.at[:, unit_block(q, m)],
                        t * G + other,
                    )
            wire.kept(3, vec_got.at[0])
            wire.settle(3, vec_got.at[pl.ds(0, G - 1)])
            vec_sum[...] = jnp.sum(vec_got[...], axis=0)

            def main_to(k):
                wire.give(9, vec_sum.at[pl.ds(0, 8)], main_all.at[t], m * owners + lax.rem(k + t, owners))

            def bias_to(k):
                owner = k // (owners // 2) * (n // 2) + m * (owners // 2) + lax.rem(k, owners // 2)
                wire.give(10, vec_sum.at[pl.ds(0, 8)], bias_all.at[t], owner)

            def units_to(k):
                wire.give(11, vec_sum.at[pl.ds(8, 8)], unit_all.at[t], (k // shares * G + m) * shares + lax.rem(k, shares))

            loop(0, owners, main_to)
            loop(0, owners, bias_to)
            loop(0, blocks * shares, units_to)
            one_own[...] = jnp.where(here == 0, result[:rows, :], result[rows:, :])
            collect.finish()
            total = attend_part[t].astype(F32)
            for k in range(groups // 2):
                total = total + part_all[k].astype(F32)
            for other in range(G):
                attend_own[other] = total[other * depth : (other + 1) * depth, :].astype(BF16)
                for p in range(3):
                    columns = pl.ds(pl.multiple_of(p * width + m * slice_width, 128), slice_width)
                    wire.give(
                        1, attend_own.at[other, :, pl.ds(p * slice_width, slice_width)], attend_all.at[:, columns], t * G + other
                    )
            wire.kept(0, expand_part.at[0])
            wire.kept(1, attend_own.at[0])
            wire.settle(0, expand_part.at[pl.ds(0, G - 1)])
            wire.settle(1, attend_own.at[pl.ds(0, G - 1)])
            for lane, place, given in (
                (9, main_all, me // owners == m),
                (10, bias_all, lax.rem(me, n // 2) // (owners // 2) == m),
                (11, unit_all, lax.rem(me // shares, G) == m),
            ):
                wire.settle_given(lane, given, place.at[pl.ds(0, groups - 1)], (place.at[0], place))
            wire.settle_given(2, me // groups == m, merge_all.at[pl.ds(0, groups - 1)], (merge_all.at[0], merge_all))
            wire.sent(4, got.at[0])
            wire.sent(5, got.at[1])
            for k in range(3):
                wire.settle(6 + k, one_all.at[k])

        one_own, one_all, attend_parts, merge_parts, main_parts, bias_parts, unit_parts, expand_whole = exchange(
            close,
            "close",
            7,
            sizes,
            12 + groups * 3 // 2,
            (
                dq_all.reshape(slice_width, group_rows),
                dpair_all,
                input_one,
                scaled_group,
                attend_slice,
                att_all,
                grad_all.reshape(group_rows, width),
                expand_parts,
                grad_expand_part.reshape(groups, G * depth, slice_units),
                second_sums,
                grad_expand_shift,
            ),
            (
                ((rows, width), F32),
                ((3, rows, width), BF16),
                ((depth, 3 * width), BF16),
                ((groups, depth, width), BF16),
                *([((groups, 8, 128), F32)] * 3),
                ((depth, hidden_units), BF16),
            ),
            scratch=[
                pltpu.VMEM((3 * slice_width, group_rows), BF16),
                pltpu.VMEM((group_rows, 3 * slice_width), BF16),
                *([pltpu.VMEM((groups, G * depth, 3 * slice_width), BF16)] * 3),
                pltpu.VMEM((groups // 2, G * depth, 3 * slice_width), BF16),
                pltpu.VMEM((G, depth, 3 * slice_width), BF16),
                pltpu.VMEM((groups, depth, width), BF16),
                pltpu.VMEM((G, depth, slice_units), BF16),
                pltpu.VMEM((16, width), F32),
                pltpu.VMEM((G, 16, 128), F32),
                pltpu.VMEM((16, 128), F32),
                pltpu.VMEM((2, pair_rows, width), BF16),
                pltpu.VMEM((2, pair_rows, width), BF16),
                pltpu.VMEM((2, pair_rows, width), BF16),
            ],
            vmem_outs=1,
        )

        def finish(
            one_own, one_all, x, grad_hidden, hidden, shrunk, gain, shift, attend, merge, expand, shrink, shrink_own, vec_main, vec_bias, vec_units,
            residual_out, input_grad, attend_out, merge_out, expand_out, shrink_out, vec_out,
        ):
            grad_one = one_own[...]
            for k in range(3):
                grad_one = grad_one + one_all[k].astype(F32)
            scaled, inverse = normalize(x[...].astype(F32))
            input_grad[...] = grad_hidden[...] + normalize_back(grad_one, scaled, inverse, gain[...])
            total = hidden[...]
            for k in range(4):
                total = total + shrunk[k].astype(F32)
            residual_out[...] = (total + shift[...]).astype(BF16)
            total = merge[0].astype(F32)
            for k in range(1, groups):
                total = total + merge[k].astype(F32)
            merge_out[...] = total
            attend_out[...] = attend[...].astype(F32)
            total = shrink_own[...].astype(F32)
            for k in range(shrink_terms):
                total = total + shrink[k].astype(F32)
            shrink_out[...] = total
            expand_out[...] = expand[...].astype(F32)

            @pl.when(pl.program_id(0) == 0)
            def _():
                for k, source in enumerate((vec_main, vec_bias, vec_units)):
                    vec_out[k] = jnp.sum(source[...], axis=0)

        turns = 4
        by_rows = pl.BlockSpec((rows // turns, width), lambda i: (i, 0))
        by_lanes = lambda r, c: pl.BlockSpec((r, c // turns), lambda i: (0, i))
        terms = lambda k: pl.BlockSpec((k, rows // turns, width), lambda i: (0, i, 0))
        terms_by_lanes = lambda k, r, c: pl.BlockSpec((k, r, c // turns), lambda i: (0, 0, i))
        small_terms = pl.BlockSpec((groups, 8, 128), lambda i: (0, 0, 0))
        line = pl.BlockSpec((1, width), lambda i: (0, 0))
        (
            residual_out, input_grad, grad_attend_weight, grad_merge_weight, grad_expand_weight, grad_shrink_weight, vec_sums,
        ) = pl.pallas_call(
            finish,
            grid=(turns,),
            out_shape=[
                jax.ShapeDtypeStruct((rows, width), BF16),
                jax.ShapeDtypeStruct((rows, width), F32),
                jax.ShapeDtypeStruct((depth, 3 * width), F32),
                jax.ShapeDtypeStruct((depth, width), F32),
                jax.ShapeDtypeStruct((depth, hidden_units), F32),
                jax.ShapeDtypeStruct((hidden_rows, width), F32),
                jax.ShapeDtypeStruct((3, 8, 128), F32),
            ],
            in_specs=[
                by_rows, terms(3), by_rows, by_rows, by_rows, terms(4), line, line,
                by_lanes(depth, 3 * width), terms_by_lanes(groups, depth, width), by_lanes(depth, hidden_units),
                terms_by_lanes(shrink_terms, hidden_rows, width), by_lanes(hidden_rows, width), small_terms, small_terms, small_terms,
            ],
            out_specs=[
                by_rows, by_rows, by_lanes(depth, 3 * width), by_lanes(depth, width), by_lanes(depth, hidden_units),
                by_lanes(hidden_rows, width), pl.BlockSpec((3, 8, 128), lambda i: (0, 0, 0)),
            ],
            name="finish",
        )(
            one_own, one_all, residual_in, grad_hidden, hidden, shrunk_parts, gain_one.reshape(1, width),
            shrink_shift.reshape(1, width), attend_parts, merge_parts, expand_whole, shrink_parts,
            shrink_own, main_parts, bias_parts, unit_parts,
        )
        own = lax.dynamic_slice_in_dim(vec_sums[0], lax.rem(me, 128 // depth) * depth, depth, 1)
        own_bias = lax.dynamic_slice_in_dim(vec_sums[1, 2:4], lax.rem(2 * me * depth, 128), 2 * depth, 1)
        own_bias = jnp.where(me < n // 2, own_bias[0], own_bias[1])
        own_units = lax.dynamic_slice_in_dim(vec_sums[2], lax.rem(me, shares) * hidden_rows, hidden_rows, 1)
        own_units = lax.dynamic_index_in_dim(own_units, me // (G * shares), 0, False)
        return (
            residual_out,
            input_grad,
            own[0],
            own[1],
            grad_attend_weight,
            own_bias,
            grad_merge_weight,
            own[4],
            own[5],
            own[6],
            grad_expand_weight,
            own_units,
            grad_shrink_weight,
            own[7],
        )

    return on_device


def solution(mesh):
    rows, line = P(("ctx", "fsdp"), None), P(("ctx", "fsdp"))
    n, fsdp = mesh.shape["ctx"] * mesh.shape["fsdp"], mesh.shape["fsdp"]
    return jax.shard_map(
        layer(n, fsdp),
        mesh=mesh,
        in_specs=(rows, line, line, rows, line, rows, line, line, line, rows, line, rows, line, rows),
        out_specs=(rows, rows, line, line, rows, line, rows, line, line, line, rows, line, rows, line),
        check_vma=False,
    )
```
